256 devices in a mesh: dom: 128 (over x, y, z), sub: 2 (over core).
Axes of the slice: x: 4, y: 4, z: 8, core: 2. Of those that a mesh axis runs over, the one named last changes fastest.
Arguments:
- old_states: bfloat16 [4096, 320], P(('dom', 'sub')), may hold values from -6 to 6
- send_elem: int32 [256, 9, 8], P(('dom', 'sub')), may hold values from -1 to 15, as said below
- recv_slot: int32 [4096, 4], P(('dom', 'sub')), may hold values from -1 to 71, as said below
- intersection_count: int32 [4096], P(('dom', 'sub')), may hold values from 1 to 4
- intersection_weight: float32 [4096, 4], P(('dom', 'sub')), may hold values from 0.1 to 1
- interior_inverse: bfloat16 [4096, 320, 320], P(('dom', 'sub')), may hold values from -0.3125 to 0.3125
- inner_coupling: bfloat16 [4096, 320, 400], P(('dom', 'sub')), may hold values from -6 to 6
- face_coupling: bfloat16 [4096, 400, 320], P(('dom', 'sub')), may hold values from -0.3125 to 0.3125
- face_mass: float32 [80, 80], replicated, may hold values from -6 to 6
- face_scale: float32 [4096, 5], P(('dom', 'sub')), may hold values from 0.5 to 2
- face_shift: int32 [4096, 5], P(('dom', 'sub')), may hold values from -4 to 4, as said below
- owner_row: int32 [256, 9, 9], P(('dom', 'sub')), may hold values from -1 to 39, as said below
Outputs:
- face_schur: float32 [10240, 6400], P(('dom', 'sub'))
- face_rhs: float32 [10240, 80], P(('dom', 'sub'))
The draws below stay inside these ranges and needn't reach their ends.
Inputs may be any that keep to these rules, and one draw needn't show every extreme that they name: `send_elem`: -1 marks an empty slot. For every live entry of recv_slot the named slot holds an element of the source; no slot is named twice; some old owner fills all 8 slots toward one new owner. `recv_slot`: entry k of new element n is -1 exactly when k >= intersection_count[n], else the index of a filled slot. `face_shift`: on one device at most 9 items share a shift value, and some value has exactly 9. `owner_row`: -1 exactly where no item arrives; every owned row is named by exactly two arriving items.
All inputs are finite; a program needn't handle non-finite values.
Results may differ from the reference program's by a relative error of at most 0.0046.
Values may be sent and summed in bfloat16 or wider, within the bound.
A program may use at most 192 MiB of HBM per device.

```python
import math
import jax
import jax.numpy as jnp
from jax import lax

NI = 320
NFACE = 5
FU = 80
K = 4
CAP = 8
REACH = 4
E_DEV = 16
NF = 400
CAPF = 9
OWNED = 40
ELEMS = 4096
FACES = 10240
N_DOM = 128
N_SUB = 2


def handover_maps(key):
    devices = N_DOM * N_SUB
    entries = E_DEV * K
    offset_count = 2 * REACH + 1
    slot_total = offset_count * CAP
    base = jax.random.fold_in(key, 11)
    perm_key, count_key, pick_key = jax.random.split(base, 3)

    def one_choice(seed_key):
        score_key, lead_key = jax.random.split(seed_key)
        scores = jax.random.permutation(score_key, slot_total).astype(jnp.int32)
        leader = jax.random.randint(lead_key, (), 0, offset_count).astype(jnp.int32)
        block_of = jnp.arange(slot_total, dtype=jnp.int32) // CAP
        scores = scores - jnp.where(block_of == leader, slot_total, 0).astype(jnp.int32)
        order = jnp.argsort(scores, stable=True).astype(jnp.int32)
        return order[:entries]
    picked = jax.vmap(one_choice)(jax.random.split(perm_key, devices))
    counts = jax.random.randint(count_key, (devices, E_DEV), 1, K + 1).astype(jnp.int32)
    full_elements = (CAP + K - 1) // K
    counts = counts.at[:, :full_elements].set(K)
    is_live = (jnp.arange(K, dtype=jnp.int32)[None, None, :] < counts[:, :, None]).reshape(devices, entries)
    receiver = jnp.arange(devices, dtype=jnp.int32)[:, None]
    offset_row = picked // CAP
    column = picked % CAP
    source = (jnp.mod(receiver // N_SUB - offset_row + REACH, N_DOM) * N_SUB + receiver % N_SUB).astype(jnp.int32)
    recv_map = jnp.where(is_live, picked, -1).astype(jnp.int32).reshape(devices * E_DEV, K)
    element = jax.random.randint(pick_key, (devices, entries), 0, E_DEV).astype(jnp.int32)
    sender_map = jnp.full((devices, offset_count, CAP), -1, jnp.int32)
    sender_map = sender_map.at[source, offset_row, column].set(jnp.where(is_live, element, -1).astype(jnp.int32))
    return (sender_map, recv_map, counts.reshape(devices * E_DEV))


def face_maps(key):
    devices = N_DOM * N_SUB
    item_count = E_DEV * NFACE
    offset_count = 2 * REACH + 1
    base = jax.random.fold_in(key, 23)
    label_key, slot_key, row_key = jax.random.split(base, 3)
    labels = jax.random.permutation(label_key, item_count).astype(jnp.int32)
    shift_list = labels % offset_count - REACH
    slot_perm = jax.vmap(lambda seed_key: jax.random.permutation(seed_key, item_count).astype(jnp.int32))(jax.random.split(slot_key, devices))
    row_rank = jax.vmap(lambda seed_key: jax.random.permutation(seed_key, item_count).astype(jnp.int32))(jax.random.split(row_key, devices))
    shift_map = jax.vmap(lambda slots: jnp.zeros((item_count,), jnp.int32).at[slots].set(shift_list))(slot_perm)
    same = shift_list[:, None] == shift_list[None, :]
    earlier = slot_perm[:, None, :] < slot_perm[:, :, None]
    ranks = jnp.sum(jnp.where(same[None] & earlier, 1, 0), axis=2).astype(jnp.int32)
    device = jnp.arange(devices, dtype=jnp.int32)[:, None]
    owner = (device // N_SUB + shift_list[None, :]) % N_DOM * N_SUB + device % N_SUB
    labels_all = jnp.broadcast_to(jnp.arange(item_count, dtype=jnp.int32)[None, :], (devices, item_count))
    rows = row_rank[owner, labels_all] // 2
    shift_all = jnp.broadcast_to(shift_list[None, :] + REACH, (devices, item_count))
    row_map = jnp.full((devices, offset_count, CAPF), -1, jnp.int32)
    row_map = row_map.at[owner, shift_all, ranks].set(rows)
    return (shift_map.reshape(devices * E_DEV, NFACE), row_map)


def draw_send_elem(key, part):
    return handover_maps(key)[0]


def draw_recv_slot(key, part):
    return handover_maps(key)[1]


def draw_intersection_count(key, part):
    return handover_maps(key)[2]


def draw_face_shift(key, part):
    return face_maps(key)[0]


def draw_owner_row(key, part):
    return face_maps(key)[1]


def level_of(own_key, dims, cuts, least, largest):
    loudness = 1.0
    for dim, parts in cuts:
        draws = jax.random.uniform(jax.random.fold_in(jax.random.fold_in(own_key, 6), dim), (parts,), jnp.float32, least / len(cuts), largest / len(cuts))
        loudness = loudness * jnp.repeat(jnp.exp(draws), dims[dim] // parts).reshape((-1,) + (1,) * (len(dims) - 1 - dim))
    return loudness


def noise(key, dims, width, bound, pieces=(), held_as=jnp.bfloat16):
    array = jax.random.normal(key, dims, jnp.float32) * width
    if len(pieces) > 0:
        array = level_of(key, dims, pieces, -0.22, 0.18) * array
    return jnp.clip(array, min=-bound, max=bound).astype(held_as)


def setup_inputs(seed: int = 0) -> dict:
    keys = jax.random.split(jax.random.key(seed), 13)
    return {
        "old_states": noise(keys[0], (ELEMS, NI), 1.0, 6.0, ((0, 256),)),
        "send_elem": draw_send_elem(jax.random.fold_in(keys[12], 71), 0),
        "recv_slot": draw_recv_slot(jax.random.fold_in(keys[12], 71), 0),
        "intersection_count": draw_intersection_count(jax.random.fold_in(keys[12], 71), 0),
        "intersection_weight": jnp.clip(jnp.exp(math.log(1.0) - 2.3025851 * jax.random.uniform(keys[4], (ELEMS, K), jnp.float32) ** level_of(keys[4], (ELEMS, K), ((0, 256),), -0.2, 0.2)), 0.1, 1.0),
        "interior_inverse": noise(keys[5], (ELEMS, NI, NI), NI ** -0.5, 0.3125, ((0, 256),)),
        "inner_coupling": noise(keys[6], (ELEMS, NI, NF), 1.0, 6.0, ((0, 256),)),
        "face_coupling": noise(keys[7], (ELEMS, NF, NI), NI ** -0.5, 0.3125, ((0, 256),)),
        "face_mass": noise(keys[8], (FU, FU), 1.0, 6.0, (), jnp.float32),
        "face_scale": jnp.clip(jnp.exp(math.log(2.0) - 1.3862944 * jax.random.uniform(keys[9], (ELEMS, NFACE), jnp.float32) ** level_of(keys[9], (ELEMS, NFACE), ((0, 256),), -0.2, 0.2)), 0.5, 2.0),
        "face_shift": draw_face_shift(jax.random.fold_in(keys[12], 71), 0),
        "owner_row": draw_owner_row(jax.random.fold_in(keys[12], 71), 0),
    }


HIGH = lax.Precision.HIGHEST


def condense_block(element_block, face_mass):
    inverse, inner_part, outer_part, source, scales = element_block
    inverse32 = inverse.astype(jnp.float32)
    mapped = jnp.einsum("eab,ebc->eac", inverse32, inner_part.astype(jnp.float32), precision=HIGH).astype(jnp.bfloat16)
    interior_load = jnp.einsum("eab,eb->ea", inverse32, source.astype(jnp.float32), precision=HIGH).astype(jnp.bfloat16)
    rows_in = outer_part.reshape(outer_part.shape[0], NFACE, FU, NI).astype(jnp.float32)
    columns = mapped.reshape(mapped.shape[0], NI, NFACE, FU).astype(jnp.float32)
    correction = jnp.einsum("ejar,erjb->ejab", rows_in, columns, precision=HIGH)
    condensed = jnp.einsum("ejar,er->eja", rows_in, interior_load.astype(jnp.float32), precision=HIGH)
    schur_block = (scales[:, :, None, None] * face_mass[None, None] - correction).astype(jnp.bfloat16)
    right_side = (-condensed).astype(jnp.bfloat16)
    return jnp.concatenate([schur_block.reshape(schur_block.shape[0], NFACE, FU * FU), right_side], axis=2)


def reference(old_states, send_elem, recv_slot, intersection_count, intersection_weight, interior_inverse, inner_coupling, face_coupling, face_mass, face_scale, face_shift, owner_row):
    devices = N_DOM * N_SUB
    new_device = (jnp.arange(ELEMS) // E_DEV).astype(jnp.int32)
    new_dom = (new_device // N_SUB).astype(jnp.int32)
    new_sub = (new_device % N_SUB).astype(jnp.int32)
    safe_slot = jnp.maximum(recv_slot, 0).astype(jnp.int32)
    offset_row = safe_slot // CAP
    source_column = safe_slot % CAP
    source_device = (jnp.mod(new_dom[:, None] - offset_row + REACH, N_DOM) * N_SUB + new_sub[:, None]).astype(jnp.int32)
    local_element = send_elem[source_device, offset_row, source_column]
    old_index = (source_device * E_DEV + jnp.maximum(local_element, 0)).astype(jnp.int32)
    states = old_states[old_index].astype(jnp.float32)
    is_live = jnp.arange(K).astype(jnp.int32)[None, :] < intersection_count[:, None]
    weights = jnp.where(is_live, intersection_weight, jnp.zeros_like(intersection_weight))
    projected = (jnp.einsum("ek,ekr->er", weights, states, precision=HIGH) / jnp.sum(weights, axis=1, keepdims=True)).astype(jnp.bfloat16)

    def one_device(element_block):
        return condense_block(element_block, face_mass)

    blocks = (interior_inverse.reshape(devices, E_DEV, NI, NI), inner_coupling.reshape(devices, E_DEV, NI, NF), face_coupling.reshape(devices, E_DEV, NF, NI), projected.reshape(devices, E_DEV, NI), face_scale.reshape(devices, E_DEV, NFACE))
    payload = lax.map(one_device, blocks)

    item_count = E_DEV * NFACE
    shifts = face_shift.reshape(devices, item_count).astype(jnp.int32)
    order = jnp.arange(item_count).astype(jnp.int32)
    same = shifts[:, :, None] == shifts[:, None, :]
    before = order[None, None, :] < order[None, :, None]
    slot_rank = jnp.sum(jnp.where(same & before, 1, 0), axis=2).astype(jnp.int32)
    device = jnp.arange(devices).astype(jnp.int32)[:, None]
    owner = (jnp.mod(device // N_SUB + shifts, N_DOM) * N_SUB + device % N_SUB).astype(jnp.int32)
    owned_rows = owner_row[owner, shifts + REACH, slot_rank]
    face_index = (owner * OWNED + owned_rows).astype(jnp.int32)
    summed = jax.ops.segment_sum(payload.reshape(devices * item_count, FU * FU + FU).astype(jnp.float32), face_index.reshape(-1), num_segments=FACES)
    return summed[:, :FU * FU], summed[:, FU * FU:]
```

```python
import functools
import jax
import jax.numpy as jnp
from jax import lax
from jax.experimental import pallas as pl
from jax.experimental.pallas import tpu as pltpu
from jax.sharding import PartitionSpec as P

F32 = jnp.float32
BF16 = jnp.bfloat16
I32 = jnp.int32
NT = (((1,), (1,)), ((), ()))
TN = (((0,), (0,)), ((), ()))


def nt(a, b):
    return lax.dot_general(a, b, NT, preferred_element_type=F32)


def offset_at(k, reach):
    half = k // 2
    odd = k % 2
    return (1 - odd) * half + odd * (2 * reach - half)


def kernel(
    dims,
    states_hbm, send_hbm, slot_hbm, count_hbm, weight_hbm, inverse_hbm, inner_hbm, outer_hbm,
    mass_hbm, scale_hbm, shift_hbm, owner_hbm,
    schur_ref, rhs_ref,
    states, send_e, slot, count, weight, inverse, inner, outer, mass, scale, shift, owner,
    mapped, source_v, source_s, st_send, st_recv, il_ref, block32, flat32, wire, arrived,
    load32, load_wire, load_arrived, spread32,
    small_sem, source_sem, inverse_sem, inner_sem, outer_sem,
    st_ssem, st_rsem, w_ssem, w_rsem, l_ssem, l_rsem,
):
    reach, n_dom, n_elem, n_face, fu, ni, cap, capf, n_k = dims
    n_off = 2 * reach + 1
    owned = schur_ref.shape[0]
    flat_rows = capf * fu * fu // 128
    item_rows = fu * fu // 128
    me = lax.axis_index("dom")

    smalls = [
        pltpu.make_async_copy(a, b, small_sem.at[q])
        for q, (a, b) in enumerate([
            (shift_hbm, shift), (scale_hbm, scale), (mass_hbm, mass), (states_hbm, states),
            (send_hbm, send_e), (slot_hbm, slot), (count_hbm, count), (weight_hbm, weight),
            (owner_hbm, owner)])
    ]
    for c in smalls:
        c.start()

    def big(n):
        rows = pl.ds(n * n_face, n_face)
        return (
            pltpu.make_async_copy(inverse_hbm.at[n], inverse.at[n], inverse_sem.at[n]),
            pltpu.make_async_copy(inner_hbm.at[rows], inner.at[rows], inner_sem.at[n]),
            pltpu.make_async_copy(outer_hbm.at[rows], outer.at[rows], outer_sem.at[n]),
        )

    @pl.loop(0, n_elem)
    def _(n):
        a, b, _c = big(n)
        a.start()
        b.start()

    @pl.loop(0, n_elem)
    def _(n):
        big(n)[2].start()

    def partner(t):
        return {"dom": lax.rem(me + t - reach + n_dom, n_dom)}

    barrier = pltpu.get_barrier_semaphore()
    for t in range(n_off):
        if t != reach:
            pl.semaphore_signal(barrier, 1, device_id=partner(t), device_id_type=pl.DeviceIdType.MESH)

    smalls[0].wait()
    sh = shift[...]
    t3 = lax.broadcasted_iota(I32, (n_off, n_face, n_elem), 0) - reach
    j3 = lax.broadcasted_iota(I32, (n_off, n_face, n_elem), 1)
    n3 = lax.broadcasted_iota(I32, (n_off, n_face, n_elem), 2)
    hit = jnp.where(jnp.broadcast_to(sh[None], (n_off, n_face, n_elem)) == t3, 1, 0)
    per_elem = jnp.sum(hit, axis=1)
    lane = lax.broadcasted_iota(I32, (n_off, n_elem), 1)
    before = jnp.zeros((n_off, n_elem), I32)
    for n in range(n_elem - 1):
        before = before + jnp.where(lane > n, jnp.broadcast_to(per_elem[:, n:n + 1], (n_off, n_elem)), 0)
    rank = jnp.broadcast_to(before[:, None, :], (n_off, n_face, n_elem))
    for j in range(n_face - 1):
        rank = rank + jnp.where(j3 > j, jnp.broadcast_to(hit[:, j:j + 1, :], (n_off, n_face, n_elem)), 0)
    code = n3 * n_face + j3
    wide = lax.broadcasted_iota(I32, (n_off, 128), 1)
    table = jnp.zeros((n_off, 128), I32)
    for r in range(capf):
        found = jnp.sum(jnp.where((hit == 1) & (rank == r), code, 0), axis=1)
        total = jnp.sum(found, axis=1, keepdims=True)
        table = jnp.where(wide == r, jnp.broadcast_to(total, (n_off, 128)), table)
    source_v[0:n_off, :] = table
    source_copy = pltpu.make_async_copy(source_v, source_s, source_sem)
    source_copy.start()

    smalls[3].wait()
    smalls[4].wait()
    old = states[...]
    picks = send_e[...]
    e_row = lax.broadcasted_iota(I32, (n_elem, cap), 0)
    for t in range(n_off):
        sel = jnp.where(e_row == jnp.broadcast_to(picks[:, t:t + 1].reshape(1, cap), (n_elem, cap)), 1.0, 0.0)
        st_send[t] = lax.dot_general(sel.astype(BF16), old, TN, preferred_element_type=F32)

    pl.semaphore_wait(barrier, n_off - 1)

    def state_copy(t):
        return pltpu.make_async_remote_copy(
            src_ref=st_send.at[t], dst_ref=st_recv.at[t], send_sem=st_ssem.at[t], recv_sem=st_rsem.at[t],
            device_id=partner(t), device_id_type=pl.DeviceIdType.MESH)

    def wire_copy(t):
        return pltpu.make_async_remote_copy(
            src_ref=wire.at[t], dst_ref=arrived.at[t], send_sem=w_ssem.at[t], recv_sem=w_rsem.at[t],
            device_id=partner(t), device_id_type=pl.DeviceIdType.MESH)

    def load_copy(t):
        return pltpu.make_async_remote_copy(
            src_ref=load_wire.at[t], dst_ref=load_arrived.at[t], send_sem=l_ssem.at[t], recv_sem=l_rsem.at[t],
            device_id=partner(t), device_id_type=pl.DeviceIdType.MESH)

    for t in range(n_off):
        if t != reach:
            state_copy(t).start()

    @pl.loop(0, n_elem)
    def _(n):
        a, b, _c = big(n)
        a.wait()
        b.wait()
        rows = pl.ds(n * n_face, n_face)
        cols = inner[rows].reshape(n_face * fu, ni)
        mapped[rows] = nt(cols, inverse[n]).astype(BF16).reshape(n_face, fu, ni)

    @pl.loop(0, n_elem)
    def _(n):
        big(n)[2].wait()

    smalls[1].wait()
    smalls[2].wait()
    source_copy.wait()
    flat32[flat_rows:, :] = jnp.zeros((flat32.shape[0] - flat_rows, 128), F32)
    load32[...] = jnp.zeros_like(load32)

    groups = capf * fu // 8
    out_rows = 8 * fu // 128

    @pl.loop(0, n_off)
    def _(k):
        t = offset_at(k, reach)
        face = mass[...]
        for r in range(capf):
            i = source_s[t, r]
            corr = nt(outer[i], mapped[i])
            block32[pl.ds(r * fu, fu), 0:fu] = scale[i % n_face, i // n_face] * face - corr
        lane_of = lax.broadcasted_iota(I32, (groups, 128), 1)
        turned = []
        for s in range(8):
            part = block32[pl.ds(s, groups, stride=8), :]
            by = (s * fu) % 128
            turned.append(pltpu.roll(part, by, 1) if by else part)
        for m in range(out_rows):
            lo, hi = m * 128, m * 128 + 128
            segs = [s for s in range(8) if s * fu < hi and (s + 1) * fu > lo]
            row = turned[segs[-1]]
            for s in reversed(segs[:-1]):
                row = jnp.where(lane_of < (s + 1) * fu - lo, turned[s], row)
            flat32[pl.ds(m, groups, stride=out_rows), :] = row
        wire[t] = flat32[...].astype(BF16)

        @pl.when(k < n_off - 1)
        def _():
            wire_copy(t).start()

    for q in (5, 6, 7, 8):
        smalls[q].wait()
    st_recv[reach] = st_send[reach]
    for t in range(n_off):
        if t != reach:
            state_copy(t).wait()
    n_slot = n_off * cap
    q_row = lax.broadcasted_iota(I32, (n_slot, n_elem), 0)
    mix = jnp.zeros((n_slot, n_elem), F32)
    live = count[...]
    for k in range(n_k):
        w = jnp.where(live > k, weight[k:k + 1, :], 0.0)
        at = jnp.broadcast_to(slot[k:k + 1, :], (n_slot, n_elem)) == q_row
        mix = mix + jnp.where(at, jnp.broadcast_to(w, (n_slot, n_elem)), 0.0)
    mix_t = jnp.transpose(mix)
    gathered = st_recv[...].reshape(n_slot, ni)
    top = jnp.dot(mix_t, gathered, precision=lax.Precision.HIGHEST, preferred_element_type=F32)
    projected = (top / jnp.sum(mix_t, axis=1, keepdims=True)).astype(BF16)
    row_of = lax.broadcasted_iota(I32, (n_elem, ni), 0)
    il_ref[...] = jnp.zeros_like(il_ref)

    @pl.loop(0, n_elem)
    def _(n):
        il_ref[...] += jnp.where(row_of == n, nt(projected, inverse[n]), 0.0)

    @pl.loop(0, n_off)
    def _(k):
        t = offset_at(k, reach)
        for r in range(capf):
            i = source_s[t, r]
            il = il_ref[pl.ds(i // n_face, 1), :].astype(BF16)
            load32[r:r + 1, 0:fu] = -nt(il, outer[i])
        load_wire[t] = load32[...].astype(BF16)

        @pl.when(k < n_off - 1)
        def _():
            load_copy(t).start()

    schur_ref[...] = jnp.zeros_like(schur_ref)
    rhs_ref[...] = jnp.zeros_like(rhs_ref)
    f_row = lax.broadcasted_iota(I32, (owned, capf), 0)
    arrived[reach] = wire[reach]
    load_arrived[reach] = load_wire[reach]
    chunk = 5

    def add_up(t):
        names = jnp.where(f_row == jnp.broadcast_to(owner[t], (owned, capf)), 1.0, 0.0).astype(BF16)
        spread32[...] = arrived[t].astype(F32)
        for b in range(0, item_rows, chunk):
            rows = jnp.concatenate(
                [spread32[pl.ds(b + d, capf, stride=item_rows), :] for d in range(chunk)], axis=1).astype(BF16)
            schur_ref[:, b * 128:(b + chunk) * 128] += jnp.dot(names, rows, preferred_element_type=F32)
        loads = load_arrived[t].astype(F32)[0:capf, 0:fu].astype(BF16)
        rhs_ref[...] += jnp.dot(names, loads, preferred_element_type=F32)

    add_up(reach)

    @pl.loop(0, n_off - 1)
    def _(k):
        t = offset_at(k, reach)
        wire_copy(t).wait_recv()
        load_copy(t).wait_recv()
        add_up(t)

    @pl.loop(0, n_off - 1)
    def _(k):
        t = offset_at(k, reach)
        wire_copy(t).wait_send()
        load_copy(t).wait_send()


def per_device(
    n_dom,
    old_states, send_elem, recv_slot, intersection_count, intersection_weight, interior_inverse,
    inner_coupling, face_coupling, face_mass, face_scale, face_shift, owner_row,
):
    n_elem, ni = old_states.shape
    n_off, cap = send_elem.shape[1:]
    capf = owner_row.shape[2]
    n_face = face_scale.shape[1]
    fu = face_mass.shape[0]
    n_k = recv_slot.shape[1]
    reach = (n_off - 1) // 2
    items = n_elem * n_face
    owned = items // 2
    wire_rows = -(-(capf * fu * fu // 128) // 16) * 16
    ins = (
        old_states,
        jnp.swapaxes(send_elem, 1, 2)[0],
        recv_slot.T,
        intersection_count.reshape(1, n_elem),
        intersection_weight.T,
        interior_inverse,
        jnp.swapaxes(inner_coupling, 1, 2).reshape(items, fu, ni),
        face_coupling.reshape(items, fu, ni),
        face_mass,
        face_scale.T,
        face_shift.T,
        jnp.swapaxes(owner_row, 0, 1),
    )
    scratch = []
    for q, a in enumerate(ins):
        space = pltpu.SMEM if q == 9 else pltpu.VMEM
        scratch.append(space(a.shape, a.dtype))
    dma = pltpu.SemaphoreType.DMA
    scratch += [
        pltpu.VMEM((items, fu, ni), BF16),
        pltpu.VMEM((16, 128), I32),
        pltpu.SMEM((16, 128), I32),
        pltpu.VMEM((n_off, cap, ni), F32),
        pltpu.VMEM((n_off, cap, ni), F32),
        pltpu.VMEM((n_elem, ni), F32),
        pltpu.VMEM((capf * fu, 128), F32),
        pltpu.VMEM((wire_rows, 128), F32),
        pltpu.VMEM((n_off, wire_rows, 128), BF16),
        pltpu.VMEM((n_off, wire_rows, 128), BF16),
        pltpu.VMEM((16, 128), F32),
        pltpu.VMEM((n_off, 16, 128), BF16),
        pltpu.VMEM((n_off, 16, 128), BF16),
        pltpu.VMEM((wire_rows, 128), F32),
        dma((9,)),
        dma(()),
        dma((n_elem,)),
        dma((n_elem,)),
        dma((n_elem,)),
    ] + [dma((n_off,)) for _ in range(6)]
    dims = (reach, n_dom, n_elem, n_face, fu, ni, cap, capf, n_k)
    return pl.pallas_call(
        functools.partial(kernel, dims),
        out_shape=(
            jax.ShapeDtypeStruct((owned, fu * fu), F32),
            jax.ShapeDtypeStruct((owned, fu), F32),
        ),
        in_specs=[pl.BlockSpec(memory_space=pl.ANY)] * len(ins),
        out_specs=(pl.BlockSpec(memory_space=pltpu.VMEM), pl.BlockSpec(memory_space=pltpu.VMEM)),
        scratch_shapes=scratch,
        compiler_params=pltpu.CompilerParams(
            collective_id=0, has_side_effects=True, vmem_limit_bytes=56 * 1024 * 1024),
        name="condense",
    )(*ins)


def solution(mesh):
    part = P(("dom", "sub"))
    in_specs = (part,) * 8 + (P(),) + (part,) * 3
    return jax.shard_map(
        functools.partial(per_device, mesh.shape["dom"]),
        mesh=mesh, in_specs=in_specs, out_specs=(part, part), check_vma=False)
```

```python
import functools
import jax
import jax.numpy as jnp
from jax import lax
from jax.experimental import pallas as pl
from jax.experimental.pallas import tpu as pltpu
from jax.sharding import PartitionSpec as P

F32 = jnp.float32
BF16 = jnp.bfloat16
I32 = jnp.int32
NT = (((1,), (1,)), ((), ()))
TN = (((0,), (0,)), ((), ()))


def nt(a, b):
    return lax.dot_general(a, b, NT, preferred_element_type=F32)


def offset_at(k, reach):
    pair = k // 2
    far = reach - pair // 2
    near = (pair + 1) // 2
    size = (1 - pair % 2) * far + (pair % 2) * near
    return reach + size * (1 - 2 * (k % 2))


def near_first(k, reach):
    return reach + (k // 2 + 1) * (1 - 2 * (k % 2))


def kernel(
    dims,
    states_hbm, send_hbm, slot_hbm, count_hbm, weight_hbm, inverse_hbm, inner_hbm, outer_hbm,
    mass_hbm, scale_hbm, shift_hbm, owner_hbm,
    schur_ref, rhs_ref,
    states, send_e, slot, count, weight, inverse, inner, outer, mass, scale, shift, owner,
    mapped, source_v, source_s, st_send, st_recv, il_ref, block32, flat32, wire, arrived,
    load32, load_wire, load_arrived, spread32,
    small_sem, source_sem, inverse_sem, inner_sem, outer_sem,
    st_ssem, st_rsem, w_ssem, w_rsem, l_ssem, l_rsem,
):
    reach, n_dom, n_elem, n_face, fu, ni, cap, capf, n_k = dims
    n_off = 2 * reach + 1
    owned = schur_ref.shape[0]
    flat_rows = capf * fu * fu // 128
    item_rows = fu * fu // 128
    me = lax.axis_index("dom")

    smalls = [
        pltpu.make_async_copy(a, b, small_sem.at[q])
        for q, (a, b) in enumerate([
            (shift_hbm, shift), (scale_hbm, scale), (mass_hbm, mass), (states_hbm, states),
            (send_hbm, send_e), (slot_hbm, slot), (count_hbm, count), (weight_hbm, weight),
            (owner_hbm, owner)])
    ]
    for c in smalls:
        c.start()

    def load_inverse(n):
        return pltpu.make_async_copy(inverse_hbm.at[n], inverse.at[n], inverse_sem.at[n])

    def load_inner(n):
        rows = pl.ds(n * n_face, n_face)
        return pltpu.make_async_copy(inner_hbm.at[rows], inner.at[rows], inner_sem.at[n])

    def load_outer(n):
        rows = pl.ds(n * n_face, n_face)
        return pltpu.make_async_copy(outer_hbm.at[rows], outer.at[rows], outer_sem.at[n])

    @pl.loop(0, n_elem)
    def _(n):
        load_inverse(n).start()
        load_inner(n).start()

    @pl.loop(0, n_elem)
    def _(n):
        load_outer(n).start()

    def partner(t):
        return {"dom": lax.rem(me + t - reach + n_dom, n_dom)}

    barrier = pltpu.get_barrier_semaphore()
    for t in range(n_off):
        if t != reach:
            pl.semaphore_signal(barrier, 1, device_id=partner(t), device_id_type=pl.DeviceIdType.MESH)

    def map_group(lo, hi):
        for n in range(lo, hi):
            load_inverse(n).wait()
            load_inner(n).wait()
        for n in range(lo, hi):
            rows = slice(n * n_face, (n + 1) * n_face)
            cols = inner[rows].reshape(n_face * fu, ni)
            mapped[rows] = nt(cols, inverse[n]).astype(BF16).reshape(n_face, fu, ni)

    starts = [0, n_elem // 8, n_elem // 4, n_elem // 2, 3 * n_elem // 4, n_elem]
    smalls[0].wait()
    smalls[3].wait()
    smalls[4].wait()
    map_group(starts[0], starts[1])

    sh = shift[...]
    t3 = lax.broadcasted_iota(I32, (n_off, n_face, n_elem), 0) - reach
    j3 = lax.broadcasted_iota(I32, (n_off, n_face, n_elem), 1)
    n3 = lax.broadcasted_iota(I32, (n_off, n_face, n_elem), 2)
    hit = jnp.where(jnp.broadcast_to(sh[None], (n_off, n_face, n_elem)) == t3, 1, 0)
    per_elem = jnp.sum(hit, axis=1)
    lane = lax.broadcasted_iota(I32, (n_off, n_elem), 1)
    before = jnp.zeros((n_off, n_elem), I32)
    for n in range(n_elem - 1):
        before = before + jnp.where(lane > n, jnp.broadcast_to(per_elem[:, n:n + 1], (n_off, n_elem)), 0)
    rank = jnp.broadcast_to(before[:, None, :], (n_off, n_face, n_elem))
    for j in range(n_face - 1):
        rank = rank + jnp.where(j3 > j, jnp.broadcast_to(hit[:, j:j + 1, :], (n_off, n_face, n_elem)), 0)
    code = n3 * n_face + j3
    wide = lax.broadcasted_iota(I32, (n_off, 128), 1)
    table = jnp.zeros((n_off, 128), I32)
    for r in range(capf):
        found = jnp.sum(jnp.where((hit == 1) & (rank == r), code, 0), axis=1)
        total = jnp.sum(found, axis=1, keepdims=True)
        table = jnp.where(wide == r, jnp.broadcast_to(total, (n_off, 128)), table)
    source_v[0:n_off, :] = table
    source_copy = pltpu.make_async_copy(source_v, source_s, source_sem)
    source_copy.start()

    old = states[...]
    picks = send_e[...]
    e_row = lax.broadcasted_iota(I32, (n_elem, cap), 0)
    for t in range(n_off):
        sel = jnp.where(e_row == jnp.broadcast_to(picks[:, t:t + 1].reshape(1, cap), (n_elem, cap)), 1.0, 0.0)
        st_send[t] = lax.dot_general(sel.astype(BF16), old, TN, preferred_element_type=F32)

    pl.semaphore_wait(barrier, n_off - 1)

    def state_copy(t):
        return pltpu.make_async_remote_copy(
            src_ref=st_send.at[t], dst_ref=st_recv.at[t], send_sem=st_ssem.at[t], recv_sem=st_rsem.at[t],
            device_id=partner(t), device_id_type=pl.DeviceIdType.MESH)

    def wire_copy(t):
        return pltpu.make_async_remote_copy(
            src_ref=wire.at[t], dst_ref=arrived.at[t], send_sem=w_ssem.at[t], recv_sem=w_rsem.at[t],
            device_id=partner(t), device_id_type=pl.DeviceIdType.MESH)

    def load_copy(t):
        return pltpu.make_async_remote_copy(
            src_ref=load_wire.at[t], dst_ref=load_arrived.at[t], send_sem=l_ssem.at[t], recv_sem=l_rsem.at[t],
            device_id=partner(t), device_id_type=pl.DeviceIdType.MESH)

    for t in range(n_off):
        if t != reach:
            state_copy(t).start()

    for lo, hi in zip(starts[1:-1], starts[2:]):
        map_group(lo, hi)

    @pl.loop(0, n_elem)
    def _(n):
        load_outer(n).wait()

    smalls[1].wait()
    smalls[2].wait()
    source_copy.wait()
    flat32[flat_rows:, :] = jnp.zeros((flat32.shape[0] - flat_rows, 128), F32)
    load32[...] = jnp.zeros_like(load32)

    groups = capf * fu // 8
    out_rows = 8 * fu // 128

    def pack(t):
        face = mass[...]
        for r in range(capf):
            i = source_s[t, r]
            corr = nt(outer[i], mapped[i])
            block32[pl.ds(r * fu, fu), 0:fu] = scale[i % n_face, i // n_face] * face - corr
        lane_of = lax.broadcasted_iota(I32, (groups, 128), 1)
        turned = []
        for s in range(8):
            part = block32[pl.ds(s, groups, stride=8), :]
            by = (s * fu) % 128
            turned.append(pltpu.roll(part, by, 1) if by else part)
        for m in range(out_rows):
            lo, hi = m * 128, m * 128 + 128
            segs = [s for s in range(8) if s * fu < hi and (s + 1) * fu > lo]
            row = turned[segs[-1]]
            for s in reversed(segs[:-1]):
                row = jnp.where(lane_of < (s + 1) * fu - lo, turned[s], row)
            flat32[pl.ds(m, groups, stride=out_rows), :] = row
        wire[t] = flat32[...].astype(BF16)

    @pl.loop(0, n_off - 1)
    def _(k):
        t = offset_at(k, reach)
        pack(t)
        wire_copy(t).start()

    pack(reach)

    for q in (5, 6, 7, 8):
        smalls[q].wait()
    st_recv[reach] = st_send[reach]
    for t in range(n_off):
        if t != reach:
            state_copy(t).wait()
    n_slot = n_off * cap
    q_row = lax.broadcasted_iota(I32, (n_slot, n_elem), 0)
    mix = jnp.zeros((n_slot, n_elem), F32)
    live = count[...]
    for k in range(n_k):
        w = jnp.where(live > k, weight[k:k + 1, :], 0.0)
        at = jnp.broadcast_to(slot[k:k + 1, :], (n_slot, n_elem)) == q_row
        mix = mix + jnp.where(at, jnp.broadcast_to(w, (n_slot, n_elem)), 0.0)
    mix_t = jnp.transpose(mix)
    gathered = st_recv[...].reshape(n_slot, ni)
    top = jnp.dot(mix_t, gathered, precision=lax.Precision.HIGHEST, preferred_element_type=F32)
    projected = (top / jnp.sum(mix_t, axis=1, keepdims=True)).astype(BF16)
    row_of = lax.broadcasted_iota(I32, (n_elem, ni), 0)
    il_ref[...] = jnp.zeros_like(il_ref)

    @pl.loop(0, n_elem)
    def _(n):
        il_ref[...] += jnp.where(row_of == n, nt(projected, inverse[n]), 0.0)

    def pack_loads(t):
        for r in range(capf):
            i = source_s[t, r]
            il = il_ref[pl.ds(i // n_face, 1), :].astype(BF16)
            load32[r:r + 1, 0:fu] = -nt(il, outer[i])
        load_wire[t] = load32[...].astype(BF16)

    @pl.loop(0, n_off - 1)
    def _(k):
        t = offset_at(k, reach)
        pack_loads(t)
        load_copy(t).start()

    pack_loads(reach)

    f_row = lax.broadcasted_iota(I32, (owned, capf), 0)
    chunk = 5

    def names(t):
        hits = f_row == jnp.broadcast_to(owner[t], (owned, capf))
        return jnp.where(hits, 1.0, 0.0).astype(BF16)

    def add_up(t, received, first):
        who = names(t)
        spread32[...] = received.astype(F32)
        for b in range(0, item_rows, chunk):
            rows = jnp.concatenate(
                [spread32[pl.ds(b + d, capf, stride=item_rows), :] for d in range(chunk)], axis=1).astype(BF16)
            part = jnp.dot(who, rows, preferred_element_type=F32)
            cols = slice(b * 128, (b + chunk) * 128)
            schur_ref[:, cols] = part if first else schur_ref[:, cols] + part

    add_up(reach, wire[reach], True)

    @pl.loop(0, n_off - 1)
    def _(k):
        t = near_first(k, reach)
        wire_copy(t).wait_recv()
        add_up(t, arrived[t], False)

    @pl.loop(0, n_off - 1)
    def _(k):
        t = near_first(k, reach)
        load_copy(t).wait_recv()

    load_arrived[reach] = load_wire[reach]
    rhs = jnp.zeros(rhs_ref.shape, F32)
    for t in range(n_off):
        loads = load_arrived[t].astype(F32)[0:capf, 0:fu].astype(BF16)
        rhs = rhs + jnp.dot(names(t), loads, preferred_element_type=F32)
    rhs_ref[...] = rhs

    @pl.loop(0, n_off - 1)
    def _(k):
        t = near_first(k, reach)
        wire_copy(t).wait_send()
        load_copy(t).wait_send()


def per_device(
    n_dom,
    old_states, send_elem, recv_slot, intersection_count, intersection_weight, interior_inverse,
    inner_coupling, face_coupling, face_mass, face_scale, face_shift, owner_row,
):
    n_elem, ni = old_states.shape
    n_off, cap = send_elem.shape[1:]
    capf = owner_row.shape[2]
    n_face = face_scale.shape[1]
    fu = face_mass.shape[0]
    n_k = recv_slot.shape[1]
    reach = (n_off - 1) // 2
    items = n_elem * n_face
    owned = items // 2
    wire_rows = -(-(capf * fu * fu // 128) // 16) * 16
    ins = (
        old_states,
        jnp.swapaxes(send_elem, 1, 2)[0],
        recv_slot.T,
        intersection_count.reshape(1, n_elem),
        intersection_weight.T,
        interior_inverse,
        jnp.swapaxes(inner_coupling, 1, 2).reshape(items, fu, ni),
        face_coupling.reshape(items, fu, ni),
        face_mass,
        face_scale.T,
        face_shift.T,
        jnp.swapaxes(owner_row, 0, 1),
    )
    scratch = []
    for q, a in enumerate(ins):
        space = pltpu.SMEM if q == 9 else pltpu.VMEM
        scratch.append(space(a.shape, a.dtype))
    dma = pltpu.SemaphoreType.DMA
    scratch += [
        pltpu.VMEM((items, fu, ni), BF16),
        pltpu.VMEM((16, 128), I32),
        pltpu.SMEM((16, 128), I32),
        pltpu.VMEM((n_off, cap, ni), F32),
        pltpu.VMEM((n_off, cap, ni), F32),
        pltpu.VMEM((n_elem, ni), F32),
        pltpu.VMEM((capf * fu, 128), F32),
        pltpu.VMEM((wire_rows, 128), F32),
        pltpu.VMEM((n_off, wire_rows, 128), BF16),
        pltpu.VMEM((n_off, wire_rows, 128), BF16),
        pltpu.VMEM((16, 128), F32),
        pltpu.VMEM((n_off, 16, 128), BF16),
        pltpu.VMEM((n_off, 16, 128), BF16),
        pltpu.VMEM((wire_rows, 128), F32),
        dma((9,)),
        dma(()),
        dma((n_elem,)),
        dma((n_elem,)),
        dma((n_elem,)),
    ] + [dma((n_off,)) for _ in range(6)]
    dims = (reach, n_dom, n_elem, n_face, fu, ni, cap, capf, n_k)
    sums = pl.pallas_call(
        functools.partial(kernel, dims),
        out_shape=(
            jax.ShapeDtypeStruct((owned, fu * fu), F32),
            jax.ShapeDtypeStruct((owned, fu), F32),
        ),
        in_specs=[pl.BlockSpec(memory_space=pltpu.HBM)] * len(ins),
        out_specs=(pl.BlockSpec(memory_space=pltpu.VMEM), pl.BlockSpec(memory_space=pltpu.VMEM)),
        scratch_shapes=scratch,
        compiler_params=pltpu.CompilerParams(
            collective_id=0, has_side_effects=True, vmem_limit_bytes=52 * 1024 * 1024),
        name="condense",
    )(*[pltpu.with_memory_space_constraint(a, pltpu.HBM) for a in ins])
    return sums


def solution(mesh):
    part = P(("dom", "sub"))
    in_specs = (part,) * 8 + (P(),) + (part,) * 3
    return jax.shard_map(
        functools.partial(per_device, mesh.shape["dom"]),
        mesh=mesh, in_specs=in_specs, out_specs=(part, part), check_vma=False)
```

```python
import functools
import jax
import jax.numpy as jnp
from jax import lax
from jax.experimental import pallas as pl
from jax.experimental.pallas import tpu as pltpu
from jax.sharding import PartitionSpec as P

F32 = jnp.float32
BF16 = jnp.bfloat16
I32 = jnp.int32
NT = (((1,), (1,)), ((), ()))
TN = (((0,), (0,)), ((), ()))


def nt(a, b):
    return lax.dot_general(a, b, NT, preferred_element_type=F32)


def offset_at(k, reach, low):
    back = k // reach
    size = reach - (k - back * reach)
    return reach + (1 - 2 * low) * (1 - 2 * back) * size


def arrival_at(k, reach, low):
    back = k // reach
    size = k - back * reach + 1
    sign = (1 - 2 * low) * (1 - 2 * back)
    return reach + sign * size


def kernel(
    dims,
    states_hbm, send_hbm, slot_hbm, count_hbm, weight_hbm, inverse_hbm, inner_hbm, outer_hbm,
    mass_hbm, scale_hbm, shift_hbm, owner_hbm,
    schur_ref, rhs_ref,
    states, send_e, slot, count, weight, inverse, inner, outer, mass, scale, shift, owner,
    mapped, source_v, source_s, st_send, st_recv, il_ref, block32, flat32, wire, arrived,
    tail32, load_wire, load_arrived, spread32,
    small_sem, source_sem, inverse_sem, inner_sem, outer_sem,
    st_ssem, st_rsem, w_ssem, w_rsem, l_ssem, l_rsem,
):
    reach, n_dom, n_elem, n_face, fu, ni, cap, capf, n_k = dims
    n_off = 2 * reach + 1
    owned = schur_ref.shape[0]
    item_rows = fu * fu // 128
    wire_rows = wire.shape[1]
    rest = capf * item_rows - wire_rows
    me = lax.axis_index("dom")
    low = 1 - lax.rem(me, 2 * reach) // reach

    smalls = [
        pltpu.make_async_copy(a, b, small_sem.at[q])
        for q, (a, b) in enumerate([
            (shift_hbm, shift), (scale_hbm, scale), (mass_hbm, mass), (states_hbm, states),
            (send_hbm, send_e), (slot_hbm, slot), (count_hbm, count), (weight_hbm, weight),
            (owner_hbm, owner)])
    ]
    starts = [0, n_elem // 8, n_elem // 4, n_elem // 2, 3 * n_elem // 4, n_elem]
    groups_of = list(zip(starts[:-1], starts[1:]))

    def load_group(g):
        lo, hi = groups_of[g]
        rows = pl.ds(lo * n_face, (hi - lo) * n_face)
        return (
            pltpu.make_async_copy(inverse_hbm.at[pl.ds(lo, hi - lo)], inverse.at[pl.ds(lo, hi - lo)], inverse_sem.at[g]),
            pltpu.make_async_copy(inner_hbm.at[rows], inner.at[rows], inner_sem.at[g]),
        )

    def load_outer(h):
        rows = pl.ds(h * n_elem * n_face // 2, n_elem * n_face // 2)
        return pltpu.make_async_copy(outer_hbm.at[rows], outer.at[rows], outer_sem.at[h])

    def start(*copies):
        for c in copies:
            c.start()

    start(*load_group(0))
    start(smalls[0], smalls[3], smalls[4])
    for g in range(1, len(groups_of)):
        start(*load_group(g))
    start(load_outer(0), load_outer(1))
    start(*(smalls[q] for q in (1, 2, 5, 6, 7, 8)))

    def partner(t):
        return {"dom": lax.rem(me + t - reach + n_dom, n_dom)}

    barrier = pltpu.get_barrier_semaphore()
    for t in range(n_off):
        if t != reach:
            pl.semaphore_signal(barrier, 1, device_id=partner(t), device_id_type=pl.DeviceIdType.MESH)

    def map_group(g):
        for c in load_group(g):
            c.wait()
        for n in range(*groups_of[g]):
            rows = slice(n * n_face, (n + 1) * n_face)
            cols = inner[rows].reshape(n_face * fu, ni)
            mapped[rows] = nt(cols, inverse[n]).astype(BF16).reshape(n_face, fu, ni)

    smalls[0].wait()
    smalls[3].wait()
    smalls[4].wait()
    map_group(0)

    sh = shift[...]
    t3 = lax.broadcasted_iota(I32, (n_off, n_face, n_elem), 0) - reach
    j3 = lax.broadcasted_iota(I32, (n_off, n_face, n_elem), 1)
    n3 = lax.broadcasted_iota(I32, (n_off, n_face, n_elem), 2)
    hit = jnp.where(jnp.broadcast_to(sh[None], (n_off, n_face, n_elem)) == t3, 1, 0)
    per_elem = jnp.sum(hit, axis=1)
    lane = lax.broadcasted_iota(I32, (n_off, n_elem), 1)
    before = jnp.zeros((n_off, n_elem), I32)
    for n in range(n_elem - 1):
        before = before + jnp.where(lane > n, jnp.broadcast_to(per_elem[:, n:n + 1], (n_off, n_elem)), 0)
    rank = jnp.broadcast_to(before[:, None, :], (n_off, n_face, n_elem))
    for j in range(n_face - 1):
        rank = rank + jnp.where(j3 > j, jnp.broadcast_to(hit[:, j:j + 1, :], (n_off, n_face, n_elem)), 0)
    code = n3 * n_face + j3
    wide = lax.broadcasted_iota(I32, (n_off, 128), 1)
    table = jnp.zeros((n_off, 128), I32)
    for r in range(capf):
        found = jnp.sum(jnp.where((hit == 1) & (rank == r), code, 0), axis=1)
        total = jnp.sum(found, axis=1, keepdims=True)
        table = jnp.where(wide == r, jnp.broadcast_to(total, (n_off, 128)), table)
    source_v[0:n_off, :] = table
    source_copy = pltpu.make_async_copy(source_v, source_s, source_sem)
    source_copy.start()

    old = states[...]
    picks = send_e[...]
    e_row = lax.broadcasted_iota(I32, (n_elem, cap), 0)
    for t in range(n_off):
        sel = jnp.where(e_row == jnp.broadcast_to(picks[:, t:t + 1].reshape(1, cap), (n_elem, cap)), 1.0, 0.0)
        st_send[t] = lax.dot_general(sel.astype(BF16), old, TN, preferred_element_type=F32)

    def state_copy(t):
        return pltpu.make_async_remote_copy(
            src_ref=st_send.at[t], dst_ref=st_recv.at[t], send_sem=st_ssem.at[t], recv_sem=st_rsem.at[t],
            device_id=partner(t), device_id_type=pl.DeviceIdType.MESH)

    def wire_copy(t):
        return pltpu.make_async_remote_copy(
            src_ref=wire.at[t], dst_ref=arrived.at[t], send_sem=w_ssem.at[t], recv_sem=w_rsem.at[t],
            device_id=partner(t), device_id_type=pl.DeviceIdType.MESH)

    def load_copy(t):
        return pltpu.make_async_remote_copy(
            src_ref=load_wire.at[t], dst_ref=load_arrived.at[t], send_sem=l_ssem.at[t], recv_sem=l_rsem.at[t],
            device_id=partner(t), device_id_type=pl.DeviceIdType.MESH)

    for g in range(1, len(groups_of)):
        map_group(g)
    load_outer(0).wait()
    load_outer(1).wait()
    smalls[1].wait()
    smalls[2].wait()
    source_copy.wait()
    tail32[...] = jnp.zeros_like(tail32)
    spread32[wire_rows:, :] = jnp.zeros((spread32.shape[0] - wire_rows, 128), F32)

    groups = capf * fu // 8
    out_rows = 8 * fu // 128

    def pack(t):
        face = mass[...]
        for r in range(capf):
            i = source_s[t, r]
            corr = nt(outer[i], mapped[i])
            block32[pl.ds(r * fu, fu), 0:fu] = scale[i % n_face, i // n_face] * face - corr
        lane_of = lax.broadcasted_iota(I32, (groups, 128), 1)
        turned = []
        for s in range(8):
            part = block32[pl.ds(s, groups, stride=8), :]
            by = (s * fu) % 128
            turned.append(pltpu.roll(part, by, 1) if by else part)
        for m in range(out_rows):
            lo, hi = m * 128, m * 128 + 128
            segs = [s for s in range(8) if s * fu < hi and (s + 1) * fu > lo]
            row = turned[segs[-1]]
            for s in reversed(segs[:-1]):
                row = jnp.where(lane_of < (s + 1) * fu - lo, turned[s], row)
            flat32[pl.ds(m, groups, stride=out_rows), :] = row
        wire[t] = flat32[0:wire_rows, :].astype(BF16)
        tail32[t, capf:capf + rest, :] = flat32[wire_rows:wire_rows + rest, :]

    pack(offset_at(0, reach, low))
    pl.semaphore_wait(barrier, n_off - 1)
    for t in range(n_off):
        if t != reach:
            state_copy(t).start()
    wire_copy(offset_at(0, reach, low)).start()

    @pl.loop(1, n_off - 1)
    def _(k):
        t = offset_at(k, reach, low)
        pack(t)
        wire_copy(t).start()

    pack(reach)

    for q in (5, 6, 7, 8):
        smalls[q].wait()
    st_recv[reach] = st_send[reach]
    for t in range(n_off):
        if t != reach:
            state_copy(t).wait()
    n_slot = n_off * cap
    q_row = lax.broadcasted_iota(I32, (n_slot, n_elem), 0)
    mix = jnp.zeros((n_slot, n_elem), F32)
    live = count[...]
    for k in range(n_k):
        w = jnp.where(live > k, weight[k:k + 1, :], 0.0)
        at = jnp.broadcast_to(slot[k:k + 1, :], (n_slot, n_elem)) == q_row
        mix = mix + jnp.where(at, jnp.broadcast_to(w, (n_slot, n_elem)), 0.0)
    mix_t = jnp.transpose(mix)
    gathered = st_recv[...].reshape(n_slot, ni)
    top = jnp.dot(mix_t, gathered, precision=lax.Precision.HIGHEST, preferred_element_type=F32)
    projected = (top / jnp.sum(mix_t, axis=1, keepdims=True)).astype(BF16)
    row_of = lax.broadcasted_iota(I32, (n_elem, ni), 0)
    il_ref[...] = jnp.zeros_like(il_ref)

    @pl.loop(0, n_elem)
    def _(n):
        il_ref[...] += jnp.where(row_of == n, nt(projected, inverse[n]), 0.0)

    def pack_loads(t):
        for r in range(capf):
            i = source_s[t, r]
            il = il_ref[pl.ds(i // n_face, 1), :].astype(BF16)
            tail32[t, r:r + 1, 0:fu] = -nt(il, outer[i])
        load_wire[t] = tail32[t].astype(BF16)

    @pl.loop(0, n_off - 1)
    def _(k):
        t = offset_at(k, reach, low)
        pack_loads(t)
        load_copy(t).start()

    pack_loads(reach)

    f_row = lax.broadcasted_iota(I32, (owned, capf), 0)
    chunk = 5

    def names(t):
        hits = f_row == jnp.broadcast_to(owner[t], (owned, capf))
        return jnp.where(hits, 1.0, 0.0).astype(BF16)

    def add_up(t, received, first):
        who = names(t)
        spread32[0:wire_rows, :] = received.astype(F32)
        for b in range(0, item_rows, chunk):
            rows = jnp.concatenate(
                [spread32[pl.ds(b + d, capf, stride=item_rows), :] for d in range(chunk)], axis=1).astype(BF16)
            part = jnp.dot(who, rows, preferred_element_type=F32)
            cols = slice(b * 128, (b + chunk) * 128)
            schur_ref[:, cols] = part if first else schur_ref[:, cols] + part

    add_up(reach, wire[reach], True)

    @pl.loop(0, n_off - 1)
    def _(k):
        t = arrival_at(k, reach, low)
        wire_copy(t).wait_recv()
        add_up(t, arrived[t], False)

    @pl.loop(0, n_off - 1)
    def _(k):
        t = arrival_at(k, reach, low)
        load_copy(t).wait_recv()

    load_arrived[reach] = load_wire[reach]
    rhs = jnp.zeros(rhs_ref.shape, F32)
    last = slice((item_rows - rest) * 128, item_rows * 128)
    ends = schur_ref[:, last]
    one_row = lax.broadcasted_iota(I32, (owned, 1), 0)
    for t in range(n_off):
        tails = load_arrived[t].astype(F32)
        rhs = rhs + jnp.dot(names(t), tails[0:capf, 0:fu].astype(BF16), preferred_element_type=F32)
        mine = jnp.where(one_row == owner[t][:, capf - 1:capf], 1.0, 0.0)
        row = jnp.concatenate([tails[capf + d:capf + d + 1, :] for d in range(rest)], axis=1)
        ends = ends + mine * row
    schur_ref[:, last] = ends
    rhs_ref[...] = rhs

    @pl.loop(0, n_off - 1)
    def _(k):
        t = arrival_at(k, reach, low)
        wire_copy(t).wait_send()
        load_copy(t).wait_send()


def write_out(schur_ref, rhs_ref, schur_hbm, rhs_hbm, sem):
    copies = [
        pltpu.make_async_copy(schur_ref, schur_hbm, sem.at[0]),
        pltpu.make_async_copy(rhs_ref, rhs_hbm, sem.at[1]),
    ]
    for c in copies:
        c.start()
    for c in copies:
        c.wait()


def per_device(
    n_dom,
    old_states, send_elem, recv_slot, intersection_count, intersection_weight, interior_inverse,
    inner_coupling, face_coupling, face_mass, face_scale, face_shift, owner_row,
):
    n_elem, ni = old_states.shape
    n_off, cap = send_elem.shape[1:]
    capf = owner_row.shape[2]
    n_face = face_scale.shape[1]
    fu = face_mass.shape[0]
    n_k = recv_slot.shape[1]
    reach = (n_off - 1) // 2
    items = n_elem * n_face
    owned = items // 2
    flat_rows = capf * fu * fu // 128
    wire_rows = flat_rows // 16 * 16
    all_rows = -(-flat_rows // 8) * 8
    ins = (
        old_states,
        jnp.swapaxes(send_elem, 1, 2)[0],
        recv_slot.T,
        intersection_count.reshape(1, n_elem),
        intersection_weight.T,
        interior_inverse,
        jnp.swapaxes(inner_coupling, 1, 2).reshape(items, fu, ni),
        face_coupling.reshape(items, fu, ni),
        face_mass,
        face_scale.T,
        face_shift.T,
        jnp.swapaxes(owner_row, 0, 1),
    )
    scratch = []
    for q, a in enumerate(ins):
        space = pltpu.SMEM if q == 9 else pltpu.VMEM
        scratch.append(space(a.shape, a.dtype))
    dma = pltpu.SemaphoreType.DMA
    scratch += [
        pltpu.VMEM((items, fu, ni), BF16),
        pltpu.VMEM((16, 128), I32),
        pltpu.SMEM((16, 128), I32),
        pltpu.VMEM((n_off, cap, ni), F32),
        pltpu.VMEM((n_off, cap, ni), F32),
        pltpu.VMEM((n_elem, ni), F32),
        pltpu.VMEM((capf * fu, 128), F32),
        pltpu.VMEM((all_rows, 128), F32),
        pltpu.VMEM((n_off, wire_rows, 128), BF16),
        pltpu.VMEM((n_off, wire_rows, 128), BF16),
        pltpu.VMEM((n_off, 16, 128), F32),
        pltpu.VMEM((n_off, 16, 128), BF16),
        pltpu.VMEM((n_off, 16, 128), BF16),
        pltpu.VMEM((all_rows, 128), F32),
        dma((9,)),
        dma(()),
        dma((n_elem,)),
        dma((n_elem,)),
        dma((n_elem,)),
    ] + [dma((n_off,)) for _ in range(6)]
    dims = (reach, n_dom, n_elem, n_face, fu, ni, cap, capf, n_k)
    sums = pl.pallas_call(
        functools.partial(kernel, dims),
        out_shape=(
            jax.ShapeDtypeStruct((owned, fu * fu), F32),
            jax.ShapeDtypeStruct((owned, fu), F32),
        ),
        in_specs=[pl.BlockSpec(memory_space=pltpu.HBM)] * len(ins),
        out_specs=(pl.BlockSpec(memory_space=pltpu.VMEM), pl.BlockSpec(memory_space=pltpu.VMEM)),
        scratch_shapes=scratch,
        compiler_params=pltpu.CompilerParams(
            collective_id=0, has_side_effects=True, vmem_limit_bytes=52 * 1024 * 1024),
        name="condense",
    )(*[pltpu.with_memory_space_constraint(a, pltpu.HBM) for a in ins])
    return pl.pallas_call(
        write_out,
        out_shape=tuple(jax.ShapeDtypeStruct(a.shape, a.dtype) for a in sums),
        in_specs=[pl.BlockSpec(memory_space=pltpu.VMEM)] * 2,
        out_specs=(pl.BlockSpec(memory_space=pltpu.HBM),) * 2,
        scratch_shapes=[dma((2,))],
        name="write_out",
    )(*[pltpu.with_memory_space_constraint(a, pltpu.VMEM) for a in sums])


def solution(mesh):
    part = P(("dom", "sub"))
    in_specs = (part,) * 8 + (P(),) + (part,) * 3
    return jax.shard_map(
        functools.partial(per_device, mesh.shape["dom"]),
        mesh=mesh, in_specs=in_specs, out_specs=(part, part), check_vma=False)
```

```python
import functools
import jax
import jax.numpy as jnp
from jax import lax
from jax.experimental import pallas as pl
from jax.experimental.pallas import tpu as pltpu
from jax.sharding import PartitionSpec as P

F32 = jnp.float32
BF16 = jnp.bfloat16
I32 = jnp.int32
NT = (((1,), (1,)), ((), ()))
TN = (((0,), (0,)), ((), ()))


def nt(a, b):
    return lax.dot_general(a, b, NT, preferred_element_type=F32)


def at_least(a, b):
    return (a - b + 64) // 64


def offset_at(k, reach, u):
    out_up = at_least(u, k)
    first = out_up * (reach - u + k) - (1 - out_up) * k
    rest = k - reach - 1
    in_up = 1 - at_least(rest, reach - 1 - u)
    second = in_up * (rest + 1) - (1 - in_up) * (rest + u - reach + 2)
    is_second = at_least(k, reach + 1)
    return reach + (1 - is_second) * first + is_second * second


def arrival_at(k, reach, u):
    near_up = 1 - at_least(k, u)
    first = near_up * (k + 1) - (1 - near_up) * (k - u + 1)
    rest = k - reach + 1
    down = at_least(u, rest)
    second = (1 - down) * rest - down * (reach - u + rest)
    is_second = at_least(k, reach - 1)
    return reach + (1 - is_second) * first + is_second * second


def kernel(
    dims,
    states_hbm, send_hbm, slot_hbm, count_hbm, weight_hbm, inverse_hbm, inner_hbm, outer_hbm,
    mass_hbm, scale_hbm, shift_hbm, owner_hbm,
    schur_ref, rhs_ref,
    states, send_e, slot, count, weight, inverse, inner, outer, mass, scale, shift, owner,
    mapped, source_v, source_s, st_send, st_recv, il_ref, all_ref, by_face, block32, flat32, wire, arrived,
    tail32, load_wire, load_arrived, spread32,
    small_sem, source_sem, inverse_sem, inner_sem, outer_sem,
    st_ssem, st_rsem, w_ssem, w_rsem, l_ssem, l_rsem,
):
    reach, n_dom, n_elem, n_face, fu, ni, cap, capf, n_k = dims
    n_off = 2 * reach + 1
    owned = schur_ref.shape[0]
    item_rows = fu * fu // 128
    wire_rows = wire.shape[1]
    rest = capf * item_rows - wire_rows
    me = lax.axis_index("dom")
    u = lax.rem(me, reach)

    smalls = [
        pltpu.make_async_copy(a, b, small_sem.at[q])
        for q, (a, b) in enumerate([
            (shift_hbm, shift), (scale_hbm, scale), (mass_hbm, mass), (states_hbm, states),
            (send_hbm, send_e), (slot_hbm, slot), (count_hbm, count), (weight_hbm, weight),
            (owner_hbm, owner)])
    ]
    starts = [0, n_elem // 8, n_elem // 4, n_elem // 2, 3 * n_elem // 4, n_elem]
    groups_of = list(zip(starts[:-1], starts[1:]))

    def load_group(g):
        lo, hi = groups_of[g]
        rows = pl.ds(lo * n_face, (hi - lo) * n_face)
        return (
            pltpu.make_async_copy(inverse_hbm.at[pl.ds(lo, hi - lo)], inverse.at[pl.ds(lo, hi - lo)], inverse_sem.at[g]),
            pltpu.make_async_copy(inner_hbm.at[rows], inner.at[rows], inner_sem.at[g]),
        )

    def load_outer(h):
        rows = pl.ds(h * n_elem * n_face // 2, n_elem * n_face // 2)
        return pltpu.make_async_copy(outer_hbm.at[rows], outer.at[rows], outer_sem.at[h])

    def start(*copies):
        for c in copies:
            c.start()

    start(*load_group(0))
    start(smalls[0], smalls[3], smalls[4])
    for g in range(1, len(groups_of)):
        start(*load_group(g))
    start(load_outer(0), load_outer(1))
    start(*(smalls[q] for q in (1, 2, 5, 6, 7, 8)))

    def partner(t):
        return {"dom": lax.rem(me + t - reach + n_dom, n_dom)}

    barrier = pltpu.get_barrier_semaphore()
    for t in range(n_off):
        if t != reach:
            pl.semaphore_signal(barrier, 1, device_id=partner(t), device_id_type=pl.DeviceIdType.MESH)

    def map_group(g):
        for c in load_group(g):
            c.wait()
        for n in range(*groups_of[g]):
            rows = slice(n * n_face, (n + 1) * n_face)
            cols = inner[rows].reshape(n_face * fu, ni)
            mapped[rows] = nt(cols, inverse[n]).astype(BF16).reshape(n_face, fu, ni)

    smalls[0].wait()
    smalls[3].wait()
    smalls[4].wait()
    map_group(0)

    sh = shift[...]
    t3 = lax.broadcasted_iota(I32, (n_off, n_face, n_elem), 0) - reach
    j3 = lax.broadcasted_iota(I32, (n_off, n_face, n_elem), 1)
    n3 = lax.broadcasted_iota(I32, (n_off, n_face, n_elem), 2)
    hit = jnp.where(jnp.broadcast_to(sh[None], (n_off, n_face, n_elem)) == t3, 1, 0)
    per_elem = jnp.sum(hit, axis=1)
    lane = lax.broadcasted_iota(I32, (n_off, n_elem), 1)
    before = jnp.zeros((n_off, n_elem), I32)
    for n in range(n_elem - 1):
        before = before + jnp.where(lane > n, jnp.broadcast_to(per_elem[:, n:n + 1], (n_off, n_elem)), 0)
    rank = jnp.broadcast_to(before[:, None, :], (n_off, n_face, n_elem))
    for j in range(n_face - 1):
        rank = rank + jnp.where(j3 > j, jnp.broadcast_to(hit[:, j:j + 1, :], (n_off, n_face, n_elem)), 0)
    code = n3 * n_face + j3
    wide = lax.broadcasted_iota(I32, (n_off, 128), 1)
    table = jnp.zeros((n_off, 128), I32)
    for r in range(capf):
        found = jnp.sum(jnp.where((hit == 1) & (rank == r), code, 0), axis=1)
        total = jnp.sum(found, axis=1, keepdims=True)
        table = jnp.where(wide == r, jnp.broadcast_to(total, (n_off, 128)), table)
    source_v[0:n_off, :] = table
    source_copy = pltpu.make_async_copy(source_v, source_s, source_sem)
    source_copy.start()

    old = states[...]
    picks = send_e[...]
    e_row = lax.broadcasted_iota(I32, (n_elem, cap), 0)
    for t in range(n_off):
        sel = jnp.where(e_row == jnp.broadcast_to(picks[:, t:t + 1].reshape(1, cap), (n_elem, cap)), 1.0, 0.0)
        st_send[t] = lax.dot_general(sel.astype(BF16), old, TN, preferred_element_type=F32)

    def state_copy(t):
        return pltpu.make_async_remote_copy(
            src_ref=st_send.at[t], dst_ref=st_recv.at[t], send_sem=st_ssem.at[t], recv_sem=st_rsem.at[t],
            device_id=partner(t), device_id_type=pl.DeviceIdType.MESH)

    def wire_copy(t):
        return pltpu.make_async_remote_copy(
            src_ref=wire.at[t], dst_ref=arrived.at[t], send_sem=w_ssem.at[t], recv_sem=w_rsem.at[t],
            device_id=partner(t), device_id_type=pl.DeviceIdType.MESH)

    def load_copy(t):
        return pltpu.make_async_remote_copy(
            src_ref=load_wire.at[t], dst_ref=load_arrived.at[t], send_sem=l_ssem.at[t], recv_sem=l_rsem.at[t],
            device_id=partner(t), device_id_type=pl.DeviceIdType.MESH)

    for g in range(1, len(groups_of)):
        map_group(g)
    load_outer(0).wait()
    load_outer(1).wait()
    smalls[1].wait()
    smalls[2].wait()
    source_copy.wait()
    tail32[...] = jnp.zeros_like(tail32)
    spread32[wire_rows:, :] = jnp.zeros((spread32.shape[0] - wire_rows, 128), F32)

    groups = capf * fu // 8
    out_rows = 8 * fu // 128

    def pack(t):
        face = mass[...]
        for r in range(capf):
            i = source_s[t, r]
            corr = nt(outer[i], mapped[i])
            block32[pl.ds(r * fu, fu), 0:fu] = scale[i % n_face, i // n_face] * face - corr
        lane_of = lax.broadcasted_iota(I32, (groups, 128), 1)
        turned = []
        for s in range(8):
            part = block32[pl.ds(s, groups, stride=8), :]
            by = (s * fu) % 128
            turned.append(pltpu.roll(part, by, 1) if by else part)
        for m in range(out_rows):
            lo, hi = m * 128, m * 128 + 128
            segs = [s for s in range(8) if s * fu < hi and (s + 1) * fu > lo]
            row = turned[segs[-1]]
            for s in reversed(segs[:-1]):
                row = jnp.where(lane_of < (s + 1) * fu - lo, turned[s], row)
            flat32[pl.ds(m, groups, stride=out_rows), :] = row
        wire[t] = flat32[0:wire_rows, :].astype(BF16)
        tail32[t, capf:capf + rest, :] = flat32[wire_rows:wire_rows + rest, :]

    pl.semaphore_wait(barrier, n_off - 1)
    for t in range(n_off):
        if t != reach:
            state_copy(t).start()
    pack(offset_at(0, reach, u))
    wire_copy(offset_at(0, reach, u)).start()

    @pl.loop(1, n_off - 1)
    def _(k):
        t = offset_at(k, reach, u)
        pack(t)
        wire_copy(t).start()

    pack(reach)

    for q in (5, 6, 7, 8):
        smalls[q].wait()
    st_recv[reach] = st_send[reach]
    for t in range(n_off):
        if t != reach:
            state_copy(t).wait()
    n_slot = n_off * cap
    q_row = lax.broadcasted_iota(I32, (n_slot, n_elem), 0)
    mix = jnp.zeros((n_slot, n_elem), F32)
    live = count[...]
    for k in range(n_k):
        w = jnp.where(live > k, weight[k:k + 1, :], 0.0)
        at = jnp.broadcast_to(slot[k:k + 1, :], (n_slot, n_elem)) == q_row
        mix = mix + jnp.where(at, jnp.broadcast_to(w, (n_slot, n_elem)), 0.0)
    mix_t = jnp.transpose(mix)
    gathered = st_recv[...].reshape(n_slot, ni)
    top = jnp.dot(mix_t, gathered, precision=lax.Precision.HIGHEST, preferred_element_type=F32)
    projected = (top / jnp.sum(mix_t, axis=1, keepdims=True)).astype(BF16)
    row_of = lax.broadcasted_iota(I32, (n_elem, ni), 0)
    il_ref[...] = jnp.zeros_like(il_ref)

    together = 4

    @pl.loop(0, n_elem // together)
    def _(g):
        part = jnp.zeros((n_elem, ni), F32)
        for d in range(together):
            n = g * together + d
            part = part + jnp.where(row_of == n, nt(projected, inverse[n]), 0.0)
        il_ref[...] += part

    il = il_ref[...].astype(BF16)
    row_nf = lax.broadcasted_iota(I32, (n_elem, n_face * fu), 0)
    all_ref[...] = jnp.zeros_like(all_ref)

    @pl.loop(0, n_elem // together)
    def _(g):
        part = jnp.zeros((n_elem, n_face * fu), F32)
        for d in range(together):
            n = g * together + d
            rows = outer[pl.ds(n * n_face, n_face)].reshape(n_face * fu, ni)
            part = part - jnp.where(row_nf == n, nt(il, rows), 0.0)
        all_ref[...] += part

    for j in range(n_face):
        by_face[j * n_elem:(j + 1) * n_elem, 0:fu] = all_ref[:, j * fu:(j + 1) * fu]

    def pack_loads(t):
        for r in range(capf):
            i = source_s[t, r]
            row = i % n_face * n_elem + i // n_face
            tail32[t, r:r + 1, 0:fu] = by_face[pl.ds(row, 1), 0:fu]
        load_wire[t] = tail32[t].astype(BF16)

    @pl.loop(0, n_off - 1)
    def _(k):
        t = offset_at(k, reach, u)
        pack_loads(t)
        load_copy(t).start()

    pack_loads(reach)

    f_row = lax.broadcasted_iota(I32, (owned, capf), 0)
    chunk = 5

    def names(t):
        hits = f_row == jnp.broadcast_to(owner[t], (owned, capf))
        return jnp.where(hits, 1.0, 0.0).astype(BF16)

    def add_up(t, received, first):
        who = names(t)
        spread32[0:wire_rows, :] = received.astype(F32)
        for b in range(0, item_rows, chunk):
            rows = jnp.concatenate(
                [spread32[pl.ds(b + d, capf, stride=item_rows), :] for d in range(chunk)], axis=1).astype(BF16)
            part = jnp.dot(who, rows, preferred_element_type=F32)
            cols = slice(b * 128, (b + chunk) * 128)
            schur_ref[:, cols] = part if first else schur_ref[:, cols] + part

    add_up(reach, wire[reach], True)

    @pl.loop(0, n_off - 1)
    def _(k):
        t = arrival_at(k, reach, u)
        wire_copy(t).wait_recv()
        add_up(t, arrived[t], False)

    @pl.loop(0, n_off - 1)
    def _(k):
        t = arrival_at(k, reach, u)
        load_copy(t).wait_recv()

    load_arrived[reach] = load_wire[reach]
    rhs = jnp.zeros(rhs_ref.shape, F32)
    last = slice((item_rows - rest) * 128, item_rows * 128)
    ends = schur_ref[:, last]
    one_row = lax.broadcasted_iota(I32, (owned, 1), 0)
    for t in range(n_off):
        tails = load_arrived[t].astype(F32)
        rhs = rhs + jnp.dot(names(t), tails[0:capf, 0:fu].astype(BF16), preferred_element_type=F32)
        mine = jnp.where(one_row == owner[t][:, capf - 1:capf], 1.0, 0.0)
        row = jnp.concatenate([tails[capf + d:capf + d + 1, :] for d in range(rest)], axis=1)
        ends = ends + mine * row
    schur_ref[:, last] = ends
    rhs_ref[...] = rhs

    @pl.loop(0, n_off - 1)
    def _(k):
        t = arrival_at(k, reach, u)
        wire_copy(t).wait_send()
        load_copy(t).wait_send()


def write_out(schur_ref, rhs_ref, schur_hbm, rhs_hbm, sem):
    copies = [
        pltpu.make_async_copy(schur_ref, schur_hbm, sem.at[0]),
        pltpu.make_async_copy(rhs_ref, rhs_hbm, sem.at[1]),
    ]
    for c in copies:
        c.start()
    for c in copies:
        c.wait()


def per_device(
    n_dom,
    old_states, send_elem, recv_slot, intersection_count, intersection_weight, interior_inverse,
    inner_coupling, face_coupling, face_mass, face_scale, face_shift, owner_row,
):
    n_elem, ni = old_states.shape
    n_off, cap = send_elem.shape[1:]
    capf = owner_row.shape[2]
    n_face = face_scale.shape[1]
    fu = face_mass.shape[0]
    n_k = recv_slot.shape[1]
    reach = (n_off - 1) // 2
    items = n_elem * n_face
    owned = items // 2
    flat_rows = capf * fu * fu // 128
    wire_rows = flat_rows // 16 * 16
    all_rows = -(-flat_rows // 8) * 8
    ins = (
        old_states,
        jnp.swapaxes(send_elem, 1, 2)[0],
        recv_slot.T,
        intersection_count.reshape(1, n_elem),
        intersection_weight.T,
        interior_inverse,
        jnp.swapaxes(inner_coupling, 1, 2).reshape(items, fu, ni),
        face_coupling.reshape(items, fu, ni),
        face_mass,
        face_scale.T,
        face_shift.T,
        jnp.swapaxes(owner_row, 0, 1),
    )
    scratch = []
    for q, a in enumerate(ins):
        space = pltpu.SMEM if q == 9 else pltpu.VMEM
        scratch.append(space(a.shape, a.dtype))
    dma = pltpu.SemaphoreType.DMA
    scratch += [
        pltpu.VMEM((items, fu, ni), BF16),
        pltpu.VMEM((16, 128), I32),
        pltpu.SMEM((16, 128), I32),
        pltpu.VMEM((n_off, cap, ni), F32),
        pltpu.VMEM((n_off, cap, ni), F32),
        pltpu.VMEM((n_elem, ni), F32),
        pltpu.VMEM((n_elem, n_face * fu), F32),
        pltpu.VMEM((items, 128), F32),
        pltpu.VMEM((capf * fu, 128), F32),
        pltpu.VMEM((all_rows, 128), F32),
        pltpu.VMEM((n_off, wire_rows, 128), BF16),
        pltpu.VMEM((n_off, wire_rows, 128), BF16),
        pltpu.VMEM((n_off, 16, 128), F32),
        pltpu.VMEM((n_off, 16, 128), BF16),
        pltpu.VMEM((n_off, 16, 128), BF16),
        pltpu.VMEM((all_rows, 128), F32),
        dma((9,)),
        dma(()),
        dma((n_elem,)),
        dma((n_elem,)),
        dma((n_elem,)),
    ] + [dma((n_off,)) for _ in range(6)]
    dims = (reach, n_dom, n_elem, n_face, fu, ni, cap, capf, n_k)
    sums = pl.pallas_call(
        functools.partial(kernel, dims),
        out_shape=(
            jax.ShapeDtypeStruct((owned, fu * fu), F32),
            jax.ShapeDtypeStruct((owned, fu), F32),
        ),
        in_specs=[pl.BlockSpec(memory_space=pltpu.HBM)] * len(ins),
        out_specs=(pl.BlockSpec(memory_space=pltpu.VMEM), pl.BlockSpec(memory_space=pltpu.VMEM)),
        scratch_shapes=scratch,
        compiler_params=pltpu.CompilerParams(
            collective_id=0, has_side_effects=True, vmem_limit_bytes=52 * 1024 * 1024),
        name="condense",
    )(*[pltpu.with_memory_space_constraint(a, pltpu.HBM) for a in ins])
    return pl.pallas_call(
        write_out,
        out_shape=tuple(jax.ShapeDtypeStruct(a.shape, a.dtype) for a in sums),
        in_specs=[pl.BlockSpec(memory_space=pltpu.VMEM)] * 2,
        out_specs=(pl.BlockSpec(memory_space=pltpu.HBM),) * 2,
        scratch_shapes=[dma((2,))],
        name="write_out",
    )(*[pltpu.with_memory_space_constraint(a, pltpu.VMEM) for a in sums])


def solution(mesh):
    part = P(("dom", "sub"))
    in_specs = (part,) * 8 + (P(),) + (part,) * 3
    return jax.shard_map(
        functools.partial(per_device, mesh.shape["dom"]),
        mesh=mesh, in_specs=in_specs, out_specs=(part, part), check_vma=False)
```

```python
import functools
import jax
import jax.numpy as jnp
from jax import lax
from jax.experimental import pallas as pl
from jax.experimental.pallas import tpu as pltpu
from jax.sharding import PartitionSpec as P

F32 = jnp.float32
BF16 = jnp.bfloat16
I32 = jnp.int32
NT = (((1,), (1,)), ((), ()))
TN = (((0,), (0,)), ((), ()))


def nt(a, b):
    return lax.dot_general(a, b, NT, preferred_element_type=F32)


def at_least(a, b):
    return (a - b + 64) // 64


def offset_at(k, reach, u):
    out_up = at_least(u, k)
    first = out_up * (reach - u + k) - (1 - out_up) * k
    rest = k - reach - 1
    in_up = 1 - at_least(rest, reach - 1 - u)
    second = in_up * (rest + 1) - (1 - in_up) * (rest + u - reach + 2)
    is_second = at_least(k, reach + 1)
    return reach + (1 - is_second) * first + is_second * second


def arrival_at(k, reach, u):
    near_up = 1 - at_least(k, u)
    first = near_up * (k + 1) - (1 - near_up) * (k - u + 1)
    rest = k - reach + 1
    down = at_least(u, rest)
    second = (1 - down) * rest - down * (reach - u + rest)
    is_second = at_least(k, reach - 1)
    return reach + (1 - is_second) * first + is_second * second


def kernel(
    dims,
    states_hbm, send_hbm, slot_hbm, count_hbm, weight_hbm, inverse_hbm, inner_hbm, outer_hbm,
    mass_hbm, scale_hbm, shift_hbm, owner_hbm,
    schur_ref, rhs_ref,
    states, send_e, slot, count, weight, inverse, inner, outer, mass, scale, shift, owner,
    mapped, source_v, source_s, st_send, st_recv, il_ref, all_ref, by_face, block32, flat32, wire, arrived,
    tail32, load_wire, load_arrived, spread32,
    small_sem, source_sem, inverse_sem, inner_sem, outer_sem,
    st_ssem, st_rsem, w_ssem, w_rsem, l_ssem, l_rsem,
):
    reach, n_dom, n_elem, n_face, fu, ni, cap, capf, n_k = dims
    n_off = 2 * reach + 1
    owned = schur_ref.shape[0]
    item_rows = fu * fu // 128
    wire_rows = wire.shape[1]
    rest = capf * item_rows - wire_rows
    me = lax.axis_index("dom")
    u = lax.rem(me, reach)

    smalls = [
        pltpu.make_async_copy(a, b, small_sem.at[q])
        for q, (a, b) in enumerate([
            (shift_hbm, shift), (scale_hbm, scale), (mass_hbm, mass), (states_hbm, states),
            (send_hbm, send_e), (slot_hbm, slot), (count_hbm, count), (weight_hbm, weight),
            (owner_hbm, owner)])
    ]
    starts = [0, n_elem // 8, n_elem // 4, n_elem // 2, 3 * n_elem // 4, n_elem]
    groups_of = list(zip(starts[:-1], starts[1:]))

    def load_group(g):
        lo, hi = groups_of[g]
        rows = pl.ds(lo * n_face, (hi - lo) * n_face)
        return (
            pltpu.make_async_copy(inverse_hbm.at[pl.ds(lo, hi - lo)], inverse.at[pl.ds(lo, hi - lo)], inverse_sem.at[g]),
            pltpu.make_async_copy(inner_hbm.at[rows], inner.at[rows], inner_sem.at[g]),
        )

    def load_outer(h):
        rows = pl.ds(h * n_elem * n_face // 2, n_elem * n_face // 2)
        return pltpu.make_async_copy(outer_hbm.at[rows], outer.at[rows], outer_sem.at[h])

    def start(*copies):
        for c in copies:
            c.start()

    start(*load_group(0))
    start(smalls[0], smalls[3], smalls[4])
    for g in range(1, len(groups_of)):
        start(*load_group(g))
    start(load_outer(0), load_outer(1))
    start(*(smalls[q] for q in (1, 2, 5, 6, 7, 8)))

    def partner(t):
        return {"dom": lax.rem(me + t - reach + n_dom, n_dom)}

    barrier = pltpu.get_barrier_semaphore()
    for t in range(n_off):
        if t != reach:
            pl.semaphore_signal(barrier, 1, device_id=partner(t), device_id_type=pl.DeviceIdType.MESH)

    def map_group(g):
        for c in load_group(g):
            c.wait()
        for n in range(*groups_of[g]):
            rows = slice(n * n_face, (n + 1) * n_face)
            cols = inner[rows].reshape(n_face * fu, ni)
            mapped[rows] = nt(cols, inverse[n]).astype(BF16).reshape(n_face, fu, ni)

    smalls[0].wait()
    smalls[3].wait()
    smalls[4].wait()
    map_group(0)

    sh = shift[...]
    t3 = lax.broadcasted_iota(I32, (n_off, n_face, n_elem), 0) - reach
    j3 = lax.broadcasted_iota(I32, (n_off, n_face, n_elem), 1)
    n3 = lax.broadcasted_iota(I32, (n_off, n_face, n_elem), 2)
    hit = jnp.where(jnp.broadcast_to(sh[None], (n_off, n_face, n_elem)) == t3, 1, 0)
    per_elem = jnp.sum(hit, axis=1)
    lane = lax.broadcasted_iota(I32, (n_off, n_elem), 1)
    before = jnp.zeros((n_off, n_elem), I32)
    for n in range(n_elem - 1):
        before = before + jnp.where(lane > n, jnp.broadcast_to(per_elem[:, n:n + 1], (n_off, n_elem)), 0)
    rank = jnp.broadcast_to(before[:, None, :], (n_off, n_face, n_elem))
    for j in range(n_face - 1):
        rank = rank + jnp.where(j3 > j, jnp.broadcast_to(hit[:, j:j + 1, :], (n_off, n_face, n_elem)), 0)
    code = n3 * n_face + j3
    wide = lax.broadcasted_iota(I32, (n_off, 128), 1)
    table = jnp.zeros((n_off, 128), I32)
    for r in range(capf):
        found = jnp.sum(jnp.where((hit == 1) & (rank == r), code, 0), axis=1)
        total = jnp.sum(found, axis=1, keepdims=True)
        table = jnp.where(wide == r, jnp.broadcast_to(total, (n_off, 128)), table)
    source_v[0:n_off, :] = table
    source_copy = pltpu.make_async_copy(source_v, source_s, source_sem)
    source_copy.start()

    old = states[...]
    picks = send_e[...]
    e_row = lax.broadcasted_iota(I32, (n_elem, cap), 0)
    for t in range(n_off):
        sel = jnp.where(e_row == jnp.broadcast_to(picks[:, t:t + 1].reshape(1, cap), (n_elem, cap)), 1.0, 0.0)
        st_send[t] = lax.dot_general(sel.astype(BF16), old, TN, preferred_element_type=F32).astype(BF16)

    def state_copy(t):
        return pltpu.make_async_remote_copy(
            src_ref=st_send.at[t], dst_ref=st_recv.at[t], send_sem=st_ssem.at[t], recv_sem=st_rsem.at[t],
            device_id=partner(t), device_id_type=pl.DeviceIdType.MESH)

    def wire_copy(t):
        return pltpu.make_async_remote_copy(
            src_ref=wire.at[t], dst_ref=arrived.at[t], send_sem=w_ssem.at[t], recv_sem=w_rsem.at[t],
            device_id=partner(t), device_id_type=pl.DeviceIdType.MESH)

    def load_copy(t):
        return pltpu.make_async_remote_copy(
            src_ref=load_wire.at[t], dst_ref=load_arrived.at[t], send_sem=l_ssem.at[t], recv_sem=l_rsem.at[t],
            device_id=partner(t), device_id_type=pl.DeviceIdType.MESH)

    for g in range(1, len(groups_of)):
        map_group(g)
    load_outer(0).wait()
    load_outer(1).wait()
    smalls[1].wait()
    smalls[2].wait()
    source_copy.wait()
    tail32[...] = jnp.zeros_like(tail32)
    spread32[wire_rows:, :] = jnp.zeros((spread32.shape[0] - wire_rows, 128), F32)

    groups = capf * fu // 8
    out_rows = 8 * fu // 128

    def pack(t):
        face = mass[...]
        for r in range(capf):
            i = source_s[t, r]
            corr = nt(outer[i], mapped[i])
            block32[pl.ds(r * fu, fu), 0:fu] = scale[i % n_face, i // n_face] * face - corr
        lane_of = lax.broadcasted_iota(I32, (groups, 128), 1)
        turned = []
        for s in range(8):
            part = block32[pl.ds(s, groups, stride=8), :]
            by = (s * fu) % 128
            turned.append(pltpu.roll(part, by, 1) if by else part)
        for m in range(out_rows):
            lo, hi = m * 128, m * 128 + 128
            segs = [s for s in range(8) if s * fu < hi and (s + 1) * fu > lo]
            row = turned[segs[-1]]
            for s in reversed(segs[:-1]):
                row = jnp.where(lane_of < (s + 1) * fu - lo, turned[s], row)
            flat32[pl.ds(m, groups, stride=out_rows), :] = row
        wire[t] = flat32[0:wire_rows, :].astype(BF16)
        tail32[t, capf:capf + rest, :] = flat32[wire_rows:wire_rows + rest, :]

    pl.semaphore_wait(barrier, n_off - 1)
    for t in range(n_off):
        if t != reach:
            state_copy(t).start()
    pack(offset_at(0, reach, u))
    wire_copy(offset_at(0, reach, u)).start()

    @pl.loop(1, n_off - 1)
    def _(k):
        t = offset_at(k, reach, u)
        pack(t)
        wire_copy(t).start()

    pack(reach)

    for q in (5, 6, 7, 8):
        smalls[q].wait()
    st_recv[reach] = st_send[reach]
    for t in range(n_off):
        if t != reach:
            state_copy(t).wait()
    n_slot = n_off * cap
    q_row = lax.broadcasted_iota(I32, (n_slot, n_elem), 0)
    mix = jnp.zeros((n_slot, n_elem), F32)
    live = count[...]
    for k in range(n_k):
        w = jnp.where(live > k, weight[k:k + 1, :], 0.0)
        at = jnp.broadcast_to(slot[k:k + 1, :], (n_slot, n_elem)) == q_row
        mix = mix + jnp.where(at, jnp.broadcast_to(w, (n_slot, n_elem)), 0.0)
    mix_t = jnp.transpose(mix)
    gathered = st_recv[...].astype(F32).reshape(n_slot, ni)
    top = jnp.dot(mix_t, gathered, precision=lax.Precision.HIGHEST, preferred_element_type=F32)
    projected = (top / jnp.sum(mix_t, axis=1, keepdims=True)).astype(BF16)
    row_of = lax.broadcasted_iota(I32, (n_elem, ni), 0)
    il_ref[...] = jnp.zeros_like(il_ref)

    together = 4

    @pl.loop(0, n_elem // together)
    def _(g):
        part = jnp.zeros((n_elem, ni), F32)
        for d in range(together):
            n = g * together + d
            part = part + jnp.where(row_of == n, nt(projected, inverse[n]), 0.0)
        il_ref[...] += part

    il = il_ref[...].astype(BF16)
    row_nf = lax.broadcasted_iota(I32, (n_elem, n_face * fu), 0)
    all_ref[...] = jnp.zeros_like(all_ref)

    @pl.loop(0, n_elem // together)
    def _(g):
        part = jnp.zeros((n_elem, n_face * fu), F32)
        for d in range(together):
            n = g * together + d
            rows = outer[pl.ds(n * n_face, n_face)].reshape(n_face * fu, ni)
            part = part - jnp.where(row_nf == n, nt(il, rows), 0.0)
        all_ref[...] += part

    for j in range(n_face):
        by_face[j * n_elem:(j + 1) * n_elem, 0:fu] = all_ref[:, j * fu:(j + 1) * fu]

    def pack_loads(t):
        for r in range(capf):
            i = source_s[t, r]
            row = i % n_face * n_elem + i // n_face
            tail32[t, r:r + 1, 0:fu] = by_face[pl.ds(row, 1), 0:fu]
        load_wire[t] = tail32[t].astype(BF16)

    @pl.loop(0, n_off - 1)
    def _(k):
        t = offset_at(k, reach, u)
        pack_loads(t)
        load_copy(t).start()

    pack_loads(reach)

    f_row = lax.broadcasted_iota(I32, (owned, capf), 0)
    chunk = 5

    def names(t):
        hits = f_row == jnp.broadcast_to(owner[t], (owned, capf))
        return jnp.where(hits, 1.0, 0.0).astype(BF16)

    def add_up(t, received, first):
        who = names(t)
        spread32[0:wire_rows, :] = received.astype(F32)
        for b in range(0, item_rows, chunk):
            rows = jnp.concatenate(
                [spread32[pl.ds(b + d, capf, stride=item_rows), :] for d in range(chunk)], axis=1).astype(BF16)
            part = jnp.dot(who, rows, preferred_element_type=F32)
            cols = slice(b * 128, (b + chunk) * 128)
            schur_ref[:, cols] = part if first else schur_ref[:, cols] + part

    add_up(reach, wire[reach], True)

    @pl.loop(0, n_off - 1)
    def _(k):
        t = arrival_at(k, reach, u)
        wire_copy(t).wait_recv()
        add_up(t, arrived[t], False)

    @pl.loop(0, n_off - 1)
    def _(k):
        t = arrival_at(k, reach, u)
        load_copy(t).wait_recv()

    load_arrived[reach] = load_wire[reach]
    rhs = jnp.zeros(rhs_ref.shape, F32)
    last = slice((item_rows - rest) * 128, item_rows * 128)
    ends = schur_ref[:, last]
    one_row = lax.broadcasted_iota(I32, (owned, 1), 0)
    for t in range(n_off):
        tails = load_arrived[t].astype(F32)
        rhs = rhs + jnp.dot(names(t), tails[0:capf, 0:fu].astype(BF16), preferred_element_type=F32)
        mine = jnp.where(one_row == owner[t][:, capf - 1:capf], 1.0, 0.0)
        row = jnp.concatenate([tails[capf + d:capf + d + 1, :] for d in range(rest)], axis=1)
        ends = ends + mine * row
    schur_ref[:, last] = ends
    rhs_ref[...] = rhs

    @pl.loop(0, n_off - 1)
    def _(k):
        t = arrival_at(k, reach, u)
        wire_copy(t).wait_send()
        load_copy(t).wait_send()


def write_out(schur_ref, rhs_ref, schur_hbm, rhs_hbm, sem):
    copies = [
        pltpu.make_async_copy(schur_ref, schur_hbm, sem.at[0]),
        pltpu.make_async_copy(rhs_ref, rhs_hbm, sem.at[1]),
    ]
    for c in copies:
        c.start()
    for c in copies:
        c.wait()


def per_device(
    n_dom,
    old_states, send_elem, recv_slot, intersection_count, intersection_weight, interior_inverse,
    inner_coupling, face_coupling, face_mass, face_scale, face_shift, owner_row,
):
    n_elem, ni = old_states.shape
    n_off, cap = send_elem.shape[1:]
    capf = owner_row.shape[2]
    n_face = face_scale.shape[1]
    fu = face_mass.shape[0]
    n_k = recv_slot.shape[1]
    reach = (n_off - 1) // 2
    items = n_elem * n_face
    owned = items // 2
    flat_rows = capf * fu * fu // 128
    wire_rows = flat_rows // 16 * 16
    all_rows = -(-flat_rows // 8) * 8
    ins = (
        old_states,
        jnp.swapaxes(send_elem, 1, 2)[0],
        recv_slot.T,
        intersection_count.reshape(1, n_elem),
        intersection_weight.T,
        interior_inverse,
        jnp.swapaxes(inner_coupling, 1, 2).reshape(items, fu, ni),
        face_coupling.reshape(items, fu, ni),
        face_mass,
        face_scale.T,
        face_shift.T,
        jnp.swapaxes(owner_row, 0, 1),
    )
    scratch = []
    for q, a in enumerate(ins):
        space = pltpu.SMEM if q == 9 else pltpu.VMEM
        scratch.append(space(a.shape, a.dtype))
    dma = pltpu.SemaphoreType.DMA
    scratch += [
        pltpu.VMEM((items, fu, ni), BF16),
        pltpu.VMEM((16, 128), I32),
        pltpu.SMEM((16, 128), I32),
        pltpu.VMEM((n_off, cap, ni), BF16),
        pltpu.VMEM((n_off, cap, ni), BF16),
        pltpu.VMEM((n_elem, ni), F32),
        pltpu.VMEM((n_elem, n_face * fu), F32),
        pltpu.VMEM((items, 128), F32),
        pltpu.VMEM((capf * fu, 128), F32),
        pltpu.VMEM((all_rows, 128), F32),
        pltpu.VMEM((n_off, wire_rows, 128), BF16),
        pltpu.VMEM((n_off, wire_rows, 128), BF16),
        pltpu.VMEM((n_off, 16, 128), F32),
        pltpu.VMEM((n_off, 16, 128), BF16),
        pltpu.VMEM((n_off, 16, 128), BF16),
        pltpu.VMEM((all_rows, 128), F32),
        dma((9,)),
        dma(()),
        dma((n_elem,)),
        dma((n_elem,)),
        dma((n_elem,)),
    ] + [dma((n_off,)) for _ in range(6)]
    dims = (reach, n_dom, n_elem, n_face, fu, ni, cap, capf, n_k)
    sums = pl.pallas_call(
        functools.partial(kernel, dims),
        out_shape=(
            jax.ShapeDtypeStruct((owned, fu * fu), F32),
            jax.ShapeDtypeStruct((owned, fu), F32),
        ),
        in_specs=[pl.BlockSpec(memory_space=pltpu.HBM)] * len(ins),
        out_specs=(pl.BlockSpec(memory_space=pltpu.VMEM), pl.BlockSpec(memory_space=pltpu.VMEM)),
        scratch_shapes=scratch,
        compiler_params=pltpu.CompilerParams(
            collective_id=0, has_side_effects=True, vmem_limit_bytes=52 * 1024 * 1024),
        name="condense",
    )(*[pltpu.with_memory_space_constraint(a, pltpu.HBM) for a in ins])
    return pl.pallas_call(
        write_out,
        out_shape=tuple(jax.ShapeDtypeStruct(a.shape, a.dtype) for a in sums),
        in_specs=[pl.BlockSpec(memory_space=pltpu.VMEM)] * 2,
        out_specs=(pl.BlockSpec(memory_space=pltpu.HBM),) * 2,
        scratch_shapes=[dma((2,))],
        name="write_out",
    )(*[pltpu.with_memory_space_constraint(a, pltpu.VMEM) for a in sums])


def solution(mesh):
    part = P(("dom", "sub"))
    in_specs = (part,) * 8 + (P(),) + (part,) * 3
    return jax.shard_map(
        functools.partial(per_device, mesh.shape["dom"]),
        mesh=mesh, in_specs=in_specs, out_specs=(part, part), check_vma=False)
```

```python
import functools
import jax
import jax.numpy as jnp
from jax import lax
from jax.experimental import pallas as pl
from jax.experimental.pallas import tpu as pltpu
from jax.sharding import PartitionSpec as P

F32 = jnp.float32
BF16 = jnp.bfloat16
I32 = jnp.int32
NT = (((1,), (1,)), ((), ()))
TN = (((0,), (0,)), ((), ()))


def nt(a, b):
    return lax.dot_general(a, b, NT, preferred_element_type=F32)


def at_least(a, b):
    return (a - b + 64) // 64


def offset_at(k, reach, u):
    out_up = at_least(u, k)
    first = out_up * (reach - u + k) - (1 - out_up) * k
    rest = k - reach - 1
    in_up = 1 - at_least(rest, reach - 1 - u)
    second = in_up * (rest + 1) - (1 - in_up) * (rest + u - reach + 2)
    is_second = at_least(k, reach + 1)
    return reach + (1 - is_second) * first + is_second * second


def arrival_at(k, reach, u):
    near_up = 1 - at_least(k, u)
    first = near_up * (k + 1) - (1 - near_up) * (k - u + 1)
    rest = k - reach + 1
    down = at_least(u, rest)
    second = (1 - down) * rest - down * (reach - u + rest)
    is_second = at_least(k, reach - 1)
    return reach + (1 - is_second) * first + is_second * second


def kernel(
    dims,
    states_hbm, send_hbm, slot_hbm, count_hbm, weight_hbm, inverse_hbm, inner_hbm, outer_hbm,
    mass_hbm, scale_hbm, shift_hbm, owner_hbm,
    schur_ref, rhs_ref,
    states, send_e, slot, count, weight, inverse, inner, outer, mass, scale, shift, owner,
    mapped, source_v, source_s, st_send, st_recv, il_ref, all_ref, by_face, block32, flat32, wire, arrived,
    tail32, load_wire, load_arrived, spread32,
    small_sem, source_sem, inverse_sem, inner_sem, outer_sem,
    st_ssem, st_rsem, w_ssem, w_rsem, l_ssem, l_rsem,
):
    reach, n_dom, n_elem, n_face, fu, ni, cap, capf, n_k = dims
    n_off = 2 * reach + 1
    owned = schur_ref.shape[0]
    item_rows = fu * fu // 128
    wire_rows = wire.shape[1]
    rest = capf * item_rows - wire_rows
    me = lax.axis_index("dom")
    u = lax.rem(me, reach)

    smalls = [
        pltpu.make_async_copy(a, b, small_sem.at[q])
        for q, (a, b) in enumerate([
            (shift_hbm, shift), (scale_hbm, scale), (mass_hbm, mass), (states_hbm, states),
            (send_hbm, send_e), (slot_hbm, slot), (count_hbm, count), (weight_hbm, weight),
            (owner_hbm, owner)])
    ]
    starts = [0, n_elem // 8, n_elem // 4, n_elem // 2, 3 * n_elem // 4, n_elem]
    groups_of = list(zip(starts[:-1], starts[1:]))

    def load_group(g):
        lo, hi = groups_of[g]
        rows = pl.ds(lo * n_face, (hi - lo) * n_face)
        return (
            pltpu.make_async_copy(inverse_hbm.at[pl.ds(lo, hi - lo)], inverse.at[pl.ds(lo, hi - lo)], inverse_sem.at[g]),
            pltpu.make_async_copy(inner_hbm.at[rows], inner.at[rows], inner_sem.at[g]),
        )

    def load_outer(h):
        rows = pl.ds(h * n_elem * n_face // 2, n_elem * n_face // 2)
        return pltpu.make_async_copy(outer_hbm.at[rows], outer.at[rows], outer_sem.at[h])

    def start(*copies):
        for c in copies:
            c.start()

    start(*load_group(0))
    start(smalls[0], smalls[3], smalls[4])
    for g in range(1, len(groups_of)):
        start(*load_group(g))
    start(load_outer(0), load_outer(1))
    start(*(smalls[q] for q in (1, 2, 5, 6, 7, 8)))

    def partner(t):
        return {"dom": lax.rem(me + t - reach + n_dom, n_dom)}

    barrier = pltpu.get_barrier_semaphore()
    for t in range(n_off):
        if t != reach:
            pl.semaphore_signal(barrier, 1, device_id=partner(t), device_id_type=pl.DeviceIdType.MESH)

    def map_group(g):
        for c in load_group(g):
            c.wait()
        for n in range(*groups_of[g]):
            rows = slice(n * n_face, (n + 1) * n_face)
            cols = inner[rows].reshape(n_face * fu, ni)
            mapped[rows] = nt(cols, inverse[n]).astype(BF16).reshape(n_face, fu, ni)

    smalls[0].wait()
    smalls[3].wait()
    smalls[4].wait()
    map_group(0)

    sh = shift[...]
    t3 = lax.broadcasted_iota(I32, (n_off, n_face, n_elem), 0) - reach
    j3 = lax.broadcasted_iota(I32, (n_off, n_face, n_elem), 1)
    n3 = lax.broadcasted_iota(I32, (n_off, n_face, n_elem), 2)
    hit = jnp.where(jnp.broadcast_to(sh[None], (n_off, n_face, n_elem)) == t3, 1, 0)
    per_elem = jnp.sum(hit, axis=1)
    lane = lax.broadcasted_iota(I32, (n_off, n_elem), 1)
    before = jnp.zeros((n_off, n_elem), I32)
    for n in range(n_elem - 1):
        before = before + jnp.where(lane > n, jnp.broadcast_to(per_elem[:, n:n + 1], (n_off, n_elem)), 0)
    rank = jnp.broadcast_to(before[:, None, :], (n_off, n_face, n_elem))
    for j in range(n_face - 1):
        rank = rank + jnp.where(j3 > j, jnp.broadcast_to(hit[:, j:j + 1, :], (n_off, n_face, n_elem)), 0)
    code = n3 * n_face + j3
    wide = lax.broadcasted_iota(I32, (n_off, 128), 1)
    table = jnp.zeros((n_off, 128), I32)
    for r in range(capf):
        found = jnp.sum(jnp.where((hit == 1) & (rank == r), code, 0), axis=1)
        total = jnp.sum(found, axis=1, keepdims=True)
        table = jnp.where(wide == r, jnp.broadcast_to(total, (n_off, 128)), table)
    source_v[0:n_off, :] = table
    source_copy = pltpu.make_async_copy(source_v, source_s, source_sem)
    source_copy.start()

    old = states[...]
    picks = send_e[...]
    e_row = lax.broadcasted_iota(I32, (n_elem, cap), 0)
    for t in range(n_off):
        sel = jnp.where(e_row == jnp.broadcast_to(picks[:, t:t + 1].reshape(1, cap), (n_elem, cap)), 1.0, 0.0)
        st_send[t] = lax.dot_general(sel.astype(BF16), old, TN, preferred_element_type=F32).astype(BF16)

    def state_copy(t):
        return pltpu.make_async_remote_copy(
            src_ref=st_send.at[t], dst_ref=st_recv.at[t], send_sem=st_ssem.at[t], recv_sem=st_rsem.at[t],
            device_id=partner(t), device_id_type=pl.DeviceIdType.MESH)

    def wire_copy(t):
        return pltpu.make_async_remote_copy(
            src_ref=wire.at[t], dst_ref=arrived.at[t], send_sem=w_ssem.at[t], recv_sem=w_rsem.at[t],
            device_id=partner(t), device_id_type=pl.DeviceIdType.MESH)

    def load_copy(t):
        return pltpu.make_async_remote_copy(
            src_ref=load_wire.at[t], dst_ref=load_arrived.at[t], send_sem=l_ssem.at[t], recv_sem=l_rsem.at[t],
            device_id=partner(t), device_id_type=pl.DeviceIdType.MESH)

    for g in range(1, len(groups_of)):
        map_group(g)
    load_outer(0).wait()
    load_outer(1).wait()
    smalls[1].wait()
    smalls[2].wait()
    source_copy.wait()
    tail32[...] = jnp.zeros_like(tail32)
    spread32[wire_rows:, :] = jnp.zeros((spread32.shape[0] - wire_rows, 128), F32)

    groups = capf * fu // 8
    out_rows = 8 * fu // 128

    def pack(t):
        face = mass[...]
        for r in range(capf):
            i = source_s[t, r]
            corr = nt(outer[i], mapped[i])
            block32[pl.ds(r * fu, fu), 0:fu] = scale[i % n_face, i // n_face] * face - corr
        lane_of = lax.broadcasted_iota(I32, (groups, 128), 1)
        turned = []
        for s in range(8):
            part = block32[pl.ds(s, groups, stride=8), :]
            by = (s * fu) % 128
            turned.append(pltpu.roll(part, by, 1) if by else part)
        for m in range(out_rows):
            lo, hi = m * 128, m * 128 + 128
            segs = [s for s in range(8) if s * fu < hi and (s + 1) * fu > lo]
            row = turned[segs[-1]]
            for s in reversed(segs[:-1]):
                row = jnp.where(lane_of < (s + 1) * fu - lo, turned[s], row)
            flat32[pl.ds(m, groups, stride=out_rows), :] = row
        wire[t] = flat32[0:wire_rows, :].astype(BF16)
        tail32[t, capf:capf + rest, :] = flat32[wire_rows:wire_rows + rest, :]

    pl.semaphore_wait(barrier, n_off - 1)
    for t in range(n_off):
        if t != reach:
            state_copy(t).start()
    pack(offset_at(0, reach, u))
    wire_copy(offset_at(0, reach, u)).start()

    @pl.loop(1, n_off - 1)
    def _(k):
        t = offset_at(k, reach, u)
        pack(t)
        wire_copy(t).start()

    pack(reach)

    for q in (5, 6, 7, 8):
        smalls[q].wait()
    st_recv[reach] = st_send[reach]
    for t in range(n_off):
        if t != reach:
            state_copy(t).wait()
    n_slot = n_off * cap
    q_row = lax.broadcasted_iota(I32, (n_slot, n_elem), 0)
    mix = jnp.zeros((n_slot, n_elem), F32)
    live = count[...]
    for k in range(n_k):
        w = jnp.where(live > k, weight[k:k + 1, :], 0.0)
        at = jnp.broadcast_to(slot[k:k + 1, :], (n_slot, n_elem)) == q_row
        mix = mix + jnp.where(at, jnp.broadcast_to(w, (n_slot, n_elem)), 0.0)
    mix_t = jnp.transpose(mix)
    gathered = st_recv[...].astype(F32).reshape(n_slot, ni)
    top = jnp.dot(mix_t, gathered, precision=lax.Precision.HIGHEST, preferred_element_type=F32)
    projected = (top / jnp.sum(mix_t, axis=1, keepdims=True)).astype(BF16)
    row_of = lax.broadcasted_iota(I32, (n_elem, ni), 0)
    il_ref[...] = jnp.zeros_like(il_ref)

    together = 8

    @pl.loop(0, n_elem // together)
    def _(g):
        part = jnp.zeros((n_elem, ni), F32)
        for d in range(together):
            n = g * together + d
            part = part + jnp.where(row_of == n, nt(projected, inverse[n]), 0.0)
        il_ref[...] += part

    il = il_ref[...].astype(BF16)
    row_nf = lax.broadcasted_iota(I32, (n_elem, n_face * fu), 0)
    all_ref[...] = jnp.zeros_like(all_ref)

    @pl.loop(0, n_elem // together)
    def _(g):
        part = jnp.zeros((n_elem, n_face * fu), F32)
        for d in range(together):
            n = g * together + d
            rows = outer[pl.ds(n * n_face, n_face)].reshape(n_face * fu, ni)
            part = part - jnp.where(row_nf == n, nt(il, rows), 0.0)
        all_ref[...] += part

    for j in range(n_face):
        by_face[j * n_elem:(j + 1) * n_elem, 0:fu] = all_ref[:, j * fu:(j + 1) * fu]

    def pack_loads(t):
        for r in range(capf):
            i = source_s[t, r]
            row = i % n_face * n_elem + i // n_face
            tail32[t, r:r + 1, 0:fu] = by_face[pl.ds(row, 1), 0:fu]
        load_wire[t] = tail32[t].astype(BF16)

    @pl.loop(0, n_off - 1)
    def _(k):
        t = offset_at(k, reach, u)
        pack_loads(t)
        load_copy(t).start()

    pack_loads(reach)

    f_row = lax.broadcasted_iota(I32, (owned, capf), 0)
    chunk = 5

    def names(t):
        hits = f_row == jnp.broadcast_to(owner[t], (owned, capf))
        return jnp.where(hits, 1.0, 0.0).astype(BF16)

    def add_up(t, received, first):
        who = names(t)
        spread32[0:wire_rows, :] = received.astype(F32)
        for b in range(0, item_rows, chunk):
            rows = jnp.concatenate(
                [spread32[pl.ds(b + d, capf, stride=item_rows), :] for d in range(chunk)], axis=1).astype(BF16)
            part = jnp.dot(who, rows, preferred_element_type=F32)
            cols = slice(b * 128, (b + chunk) * 128)
            schur_ref[:, cols] = part if first else schur_ref[:, cols] + part

    add_up(reach, wire[reach], True)

    @pl.loop(0, n_off - 1)
    def _(k):
        t = arrival_at(k, reach, u)
        wire_copy(t).wait_recv()
        add_up(t, arrived[t], False)

    @pl.loop(0, n_off - 1)
    def _(k):
        t = arrival_at(k, reach, u)
        load_copy(t).wait_recv()

    load_arrived[reach] = load_wire[reach]
    rhs = jnp.zeros(rhs_ref.shape, F32)
    last = slice((item_rows - rest) * 128, item_rows * 128)
    ends = schur_ref[:, last]
    one_row = lax.broadcasted_iota(I32, (owned, 1), 0)
    for t in range(n_off):
        tails = load_arrived[t].astype(F32)
        rhs = rhs + jnp.dot(names(t), tails[0:capf, 0:fu].astype(BF16), preferred_element_type=F32)
        mine = jnp.where(one_row == owner[t][:, capf - 1:capf], 1.0, 0.0)
        row = jnp.concatenate([tails[capf + d:capf + d + 1, :] for d in range(rest)], axis=1)
        ends = ends + mine * row
    schur_ref[:, last] = ends
    rhs_ref[...] = rhs

    @pl.loop(0, n_off - 1)
    def _(k):
        t = arrival_at(k, reach, u)
        wire_copy(t).wait_send()
        load_copy(t).wait_send()


def write_out(schur_ref, rhs_ref, schur_hbm, rhs_hbm, sem):
    copies = [
        pltpu.make_async_copy(schur_ref, schur_hbm, sem.at[0]),
        pltpu.make_async_copy(rhs_ref, rhs_hbm, sem.at[1]),
    ]
    for c in copies:
        c.start()
    for c in copies:
        c.wait()


def per_device(
    n_dom,
    old_states, send_elem, recv_slot, intersection_count, intersection_weight, interior_inverse,
    inner_coupling, face_coupling, face_mass, face_scale, face_shift, owner_row,
):
    n_elem, ni = old_states.shape
    n_off, cap = send_elem.shape[1:]
    capf = owner_row.shape[2]
    n_face = face_scale.shape[1]
    fu = face_mass.shape[0]
    n_k = recv_slot.shape[1]
    reach = (n_off - 1) // 2
    items = n_elem * n_face
    owned = items // 2
    flat_rows = capf * fu * fu // 128
    wire_rows = flat_rows // 16 * 16
    all_rows = -(-flat_rows // 8) * 8
    ins = (
        old_states,
        jnp.swapaxes(send_elem, 1, 2)[0],
        recv_slot.T,
        intersection_count.reshape(1, n_elem),
        intersection_weight.T,
        interior_inverse,
        jnp.swapaxes(inner_coupling, 1, 2).reshape(items, fu, ni),
        face_coupling.reshape(items, fu, ni),
        face_mass,
        face_scale.T,
        face_shift.T,
        jnp.swapaxes(owner_row, 0, 1),
    )
    scratch = []
    for q, a in enumerate(ins):
        space = pltpu.SMEM if q == 9 else pltpu.VMEM
        scratch.append(space(a.shape, a.dtype))
    dma = pltpu.SemaphoreType.DMA
    scratch += [
        pltpu.VMEM((items, fu, ni), BF16),
        pltpu.VMEM((16, 128), I32),
        pltpu.SMEM((16, 128), I32),
        pltpu.VMEM((n_off, cap, ni), BF16),
        pltpu.VMEM((n_off, cap, ni), BF16),
        pltpu.VMEM((n_elem, ni), F32),
        pltpu.VMEM((n_elem, n_face * fu), F32),
        pltpu.VMEM((items, 128), F32),
        pltpu.VMEM((capf * fu, 128), F32),
        pltpu.VMEM((all_rows, 128), F32),
        pltpu.VMEM((n_off, wire_rows, 128), BF16),
        pltpu.VMEM((n_off, wire_rows, 128), BF16),
        pltpu.VMEM((n_off, 16, 128), F32),
        pltpu.VMEM((n_off, 16, 128), BF16),
        pltpu.VMEM((n_off, 16, 128), BF16),
        pltpu.VMEM((all_rows, 128), F32),
        dma((9,)),
        dma(()),
        dma((n_elem,)),
        dma((n_elem,)),
        dma((n_elem,)),
    ] + [dma((n_off,)) for _ in range(6)]
    dims = (reach, n_dom, n_elem, n_face, fu, ni, cap, capf, n_k)
    sums = pl.pallas_call(
        functools.partial(kernel, dims),
        out_shape=(
            jax.ShapeDtypeStruct((owned, fu * fu), F32),
            jax.ShapeDtypeStruct((owned, fu), F32),
        ),
        in_specs=[pl.BlockSpec(memory_space=pltpu.HBM)] * len(ins),
        out_specs=(pl.BlockSpec(memory_space=pltpu.VMEM), pl.BlockSpec(memory_space=pltpu.VMEM)),
        scratch_shapes=scratch,
        compiler_params=pltpu.CompilerParams(
            collective_id=0, has_side_effects=True, vmem_limit_bytes=52 * 1024 * 1024),
        name="condense",
    )(*[pltpu.with_memory_space_constraint(a, pltpu.HBM) for a in ins])
    return pl.pallas_call(
        write_out,
        out_shape=tuple(jax.ShapeDtypeStruct(a.shape, a.dtype) for a in sums),
        in_specs=[pl.BlockSpec(memory_space=pltpu.VMEM)] * 2,
        out_specs=(pl.BlockSpec(memory_space=pltpu.HBM),) * 2,
        scratch_shapes=[dma((2,))],
        name="write_out",
    )(*[pltpu.with_memory_space_constraint(a, pltpu.VMEM) for a in sums])


def solution(mesh):
    part = P(("dom", "sub"))
    in_specs = (part,) * 8 + (P(),) + (part,) * 3
    return jax.shard_map(
        functools.partial(per_device, mesh.shape["dom"]),
        mesh=mesh, in_specs=in_specs, out_specs=(part, part), check_vma=False)
```
